32 devices in a mesh: expert: 8 (over z, y), half: 4 (over x, core).
Axes of the slice: x: 2, y: 2, z: 4, core: 2. Of those that a mesh axis runs over, the one named last changes fastest.
Arguments:
- tokens: bfloat16 [1024, 2048], P('expert', 'half'), may hold values from -6 to 6
- cotangent: bfloat16 [1024, 2048], P('expert', 'half'), may hold values from -4 to 4
- route: int32 [1024, 8], P('expert'), may hold values from 0 to 15, all different within a row; in each aligned block of 128 rows (0 to 127, 128 to 255, ...) at most 128 rows name the same one
- prob: bfloat16 [1024, 8], P('expert'), may hold values from 0.19921875 to 1
- w_gate: bfloat16 [16, 768, 2048], P('expert', 'half'), may hold values from -0.125 to 0.125
- w_up: bfloat16 [16, 768, 2048], P('expert', 'half'), may hold values from -0.125 to 0.125
- w_down: bfloat16 [16, 768, 2048], P('expert', 'half'), may hold values from -0.21875 to 0.21875
Outputs:
- grad_tokens: bfloat16 [1024, 2048], P('expert', 'half')
- grad_prob: float32 [1024, 8], P('expert')
- grad_gate: bfloat16 [16, 768, 2048], P('expert', 'half')
- grad_up: bfloat16 [16, 768, 2048], P('expert', 'half')
- grad_down: bfloat16 [16, 768, 2048], P('expert', 'half')
The draws below stay inside these ranges and needn't reach their ends.
Inputs may be any that keep to these rules, and one draw needn't show every extreme that they name: `route`: each row names 8 different experts; among the rows of one device no expert is named more than 128 times, and that most is reached.
All inputs are finite; a program needn't handle non-finite values.
Results may differ from the reference program's by a relative error of at most 0.013.
Values may be sent and summed in bfloat16 or wider, within the bound.
A program may use at most 192 MiB of HBM per device.

```python
import math
import jax
import jax.numpy as jnp
import numpy as np
from jax import lax

D = 2048
FF = 768
K = 8
TOK_DEV = 128
E = 16
TOKENS = 1024
CAP = 128
N_EXPERT = 8
N_HALF = 4


def block_levels(key, extent, split, smallest, top_value):
    loudness, own = 1.0, jax.random.fold_in(key, 6)
    for position, blocks in split:
        steps = jnp.exp(jax.random.uniform(jax.random.fold_in(own, position), (blocks,), jnp.float32, smallest / len(split), top_value / len(split)))
        loudness = loudness * jnp.repeat(steps, extent[position] // blocks).reshape([-1 if axis == position else 1 for axis in range(len(extent))])
    return loudness


def shared_out(key, own, number, rows, number_of, top, limit, lean):
    order = jax.random.permutation(key, number_of)
    packed, usual = load_shares(number_of, rows * top, limit, lean, True), load_shares(number_of, rows * top, limit, lean, False)
    places = jnp.arange(number_of)

    def named(sizes, offset_by):
        used = int((sizes > 0).sum())
        fixed = max(1, used // 4)
        shifted = fixed + (places - fixed + offset_by * (used - fixed)) % max(1, number_of - fixed)
        return jnp.zeros((number_of,), jnp.int32).at[order[jnp.where(places < fixed, places, shifted)]].set(jnp.asarray(sizes, jnp.int32))

    sizes = jnp.where(number % 4 == 0, named(packed, number // 4), named(usual, number - number // 4 - 1))
    mixed = jax.random.permutation(jax.random.fold_in(own, 3), number_of)
    giver, sink = mixed[0:number_of // 2 * 2:2], mixed[1:number_of // 2 * 2:2]
    margin = jnp.minimum(sizes[giver] - 1, limit - sizes[sink]) // 2
    margin = jnp.where((giver == order[0]) | (sink == order[0]) | (sizes[sink] == 0), 0, jnp.maximum(margin, 0))
    shifted = jax.random.randint(jax.random.fold_in(own, 4), (number_of // 2,), 0, 1 << 20) % (margin + 1)
    sizes = sizes.at[giver].add(-shifted).at[sink].add(shifted)
    members = jnp.searchsorted(jnp.cumsum(sizes), jnp.arange(rows * top), side="right").astype(jnp.int32)
    table = members.reshape(top, rows).T
    table = table[jax.random.permutation(jax.random.fold_in(own, 1), rows)]
    offset_by = jax.random.randint(jax.random.fold_in(own, 2), (rows, 1), 0, top)
    return jnp.take_along_axis(table, (jnp.arange(top)[None, :] + offset_by) % top, axis=1)


def load_shares(number_of, total, reach, skew, full):
    loads = [(1 << 20) // math.isqrt(rank ** skew) + 1 for rank in range(1, number_of + 1)]
    largest = reach if full else min(reach, max(-(-total // number_of), total * loads[0] // sum(loads)))
    least = 1 if total - largest >= number_of - 1 else 0
    counts, rest = [largest] + [least] * (number_of - 1), total - largest - least * (number_of - 1)
    while rest > 0:
        movable = [i for i in range(1, number_of) if counts[i] < largest] or [i for i in range(1, number_of) if counts[i] < reach]
        whole, budget = sum([loads[i] for i in movable]), rest
        for i in movable:
            more = min(reach - counts[i], max(1, budget * loads[i] // whole), rest)
            counts[i] = counts[i] + more
            rest = rest - more
    return np.array(counts)


def bell_draw(rng, shape, scale, bound, split=(), kind=jnp.bfloat16):
    array = scale * jax.random.normal(rng, shape, jnp.float32)
    if split:
        array = array * block_levels(rng, shape, split, -0.22, 0.18)
    return jnp.clip(array, -bound, bound).astype(kind)


def setup_inputs(seed: int = 0) -> dict:
    key_of = jax.random.split(jax.random.key(seed), 8)
    tokens = bell_draw(key_of[0], (TOKENS, D), 1.0, 6.0, ((0, 8), (1, 4)))
    cotangent = bell_draw(key_of[1], (TOKENS, D), 0.5, 4.0, ((0, 8), (1, 4)))
    route_keys = jax.random.split(jax.random.fold_in(key_of[2], 1), TOKENS // TOK_DEV)
    route_turns = jax.random.permutation(jax.random.fold_in(key_of[2], 3), TOKENS // TOK_DEV)
    route = jax.vmap(lambda own, number: shared_out(jax.random.fold_in(key_of[2], 2), own, number, TOK_DEV, E, K, CAP, 2))(route_keys, route_turns).reshape((TOKENS, K))
    prob = jnp.clip(0.19921875 + 0.80078125 * jax.random.uniform(key_of[3], (TOKENS, K), jnp.float32) ** block_levels(key_of[3], (TOKENS, K), ((0, 8),), -0.2, 0.2), 0.19921875, 1.0).astype(jnp.bfloat16)
    w_gate = bell_draw(key_of[4], (E, FF, D), D ** -0.5, 0.125, ((0, 8), (1, 4)))
    w_up = bell_draw(key_of[5], (E, FF, D), D ** -0.5, 0.125, ((0, 8), (1, 4)))
    w_down = bell_draw(key_of[6], (E, FF, D), FF ** -0.5, 0.21875, ((0, 8), (1, 4)))
    return dict(tokens=tokens, cotangent=cotangent, route=route, prob=prob, w_gate=w_gate, w_up=w_up, w_down=w_down)


def reference(tokens, cotangent, route, prob, w_gate, w_up, w_down):
    flat_route = route.reshape(-1)
    flat_prob = prob.reshape(-1).astype(jnp.float32)
    rows_max = N_EXPERT * CAP
    count = TOKENS * K
    order = jnp.arange(count, dtype=jnp.int32)
    quarter = FF // N_HALF

    def one_expert(carry, expert):
        grad_in, grad_weight = carry
        chosen = flat_route == expert
        place = jnp.where(chosen, jnp.cumsum(chosen.astype(jnp.int32)) - 1, rows_max).astype(jnp.int32)
        source = jnp.zeros((rows_max,), jnp.int32).at[place].set(order, mode="drop")
        filled = jnp.zeros((rows_max,), jnp.float32).at[place].set(1.0, mode="drop")
        token_of = (source // K).astype(jnp.int32)
        keep = filled[:, None] > 0.5
        xin = jnp.where(keep, tokens[token_of], jnp.zeros((), jnp.bfloat16))
        dout = jnp.where(keep, cotangent[token_of], jnp.zeros((), jnp.bfloat16))
        weight = flat_prob[source] * filled
        wgate = w_gate[expert]
        wup = w_up[expert]
        wdown = w_down[expert]
        gate = jnp.dot(xin, wgate.T, preferred_element_type=jnp.float32)
        upval = jnp.dot(xin, wup.T, preferred_element_type=jnp.float32)
        sig = jax.nn.sigmoid(gate)
        act = gate * sig
        hidden = (act * upval).astype(jnp.bfloat16)
        raw = jnp.dot(dout, wdown.T, preferred_element_type=jnp.float32)
        score = jnp.sum(hidden.astype(jnp.float32) * raw, axis=1)
        scaled = (weight[:, None] * dout.astype(jnp.float32)).astype(jnp.bfloat16)
        dact = weight[:, None] * raw
        dgate = (dact * upval * sig * (1.0 + gate * (1.0 - sig))).astype(jnp.bfloat16)
        dup = (dact * act).astype(jnp.bfloat16)
        grad_down = jnp.dot(hidden.T, scaled, preferred_element_type=jnp.float32).astype(jnp.bfloat16)
        grad_gate = jnp.dot(dgate.T, xin, preferred_element_type=jnp.float32).astype(jnp.bfloat16)
        grad_up = jnp.dot(dup.T, xin, preferred_element_type=jnp.float32).astype(jnp.bfloat16)
        dgate_f = dgate.astype(jnp.float32).reshape(rows_max, N_HALF, quarter)
        dup_f = dup.astype(jnp.float32).reshape(rows_max, N_HALF, quarter)
        wgate_f = wgate.astype(jnp.float32).reshape(N_HALF, quarter, D)
        wup_f = wup.astype(jnp.float32).reshape(N_HALF, quarter, D)
        parts = jnp.einsum("rhf,hfd->hrd", dgate_f, wgate_f) + jnp.einsum("rhf,hfd->hrd", dup_f, wup_f)
        parts = parts.astype(jnp.bfloat16).astype(jnp.float32)
        part_sum = jnp.sum(parts, axis=0) * filled[:, None]
        grad_in = grad_in.at[token_of].add(part_sum)
        grad_weight = grad_weight.at[source].add(score * filled)
        return (grad_in, grad_weight), (grad_gate, grad_up, grad_down)

    start = (jnp.zeros((TOKENS, D), jnp.float32), jnp.zeros((count,), jnp.float32))
    (grad_in, grad_weight), (grad_gate, grad_up, grad_down) = lax.scan(one_expert, start, jnp.arange(E, dtype=jnp.int32))
    return grad_in.astype(jnp.bfloat16), grad_weight.reshape(TOKENS, K), grad_gate, grad_up, grad_down
```

```python
import functools

import jax
import jax.numpy as jnp
from jax import lax
from jax.experimental import pallas as pl
from jax.experimental.pallas import tpu as pltpu
from jax.sharding import PartitionSpec as P

BOTH = ("expert", "half")


def gather_all(block, groups, halves):
    rows, quarter = block.shape
    parts = lax.all_gather(block, BOTH, axis=0).reshape(groups, halves, rows, quarter)
    return parts.transpose(0, 2, 1, 3).reshape(groups * rows, halves * quarter)


LANES = 128
VMEM_BYTES = 48 << 20
MESH = pl.DeviceIdType.MESH


def place(groups):
    e, h = lax.axis_index("expert"), lax.axis_index("half")
    return lax.div(e, 2), lax.rem(e, 2), lax.div(h, 2), lax.rem(h, 2)


def across(z, step):
    bit = 1
    while bit <= step:
        if step & bit:
            z = z + bit * (1 - 2 * lax.rem(lax.div(z, bit), 2))
        bit *= 2
    return z


def greet(peers):
    barrier = pltpu.get_barrier_semaphore()
    for peer in peers:
        pl.semaphore_signal(barrier, inc=1, device_id=peer, device_id_type=MESH)
    pl.semaphore_wait(barrier, len(peers))


def fused_kernel(
    groups, halves, local_exp, tok_ref, cot_ref, route_ref, prob_ref, wg_ref, wu_ref, wd_ref,
    gt_ref, gp_ref, gg_ref, gu_ref, gd_ref,
    xb, db, wgu, wdn, gates, raws, dgu, hps, turned, tab_own, tab_in, score, back,
    psend, own, cin, acc, xin0, yin0, yin1, xin1, t0, t1, fin, zin,
    first_send, second_send, core_send, z_send, z_sem, p_sem, q_sem, c_sem, own_sem, w_sem,
    tab_send, tab_recv, score_send, score_recv,
    part_send, part_recv, hop_send, hop_recv, last_send, last_recv,
):
    line = groups // 2
    z, y, x, c = place(groups)
    e, h = 2 * z + y, 2 * x + c
    rows, quarter = tok_ref.shape
    wide = quarter // 2
    hidden_rows, width = wg_ref.shape
    units = hidden_rows // local_exp
    experts = local_exp * groups
    top = route_ref.shape[1]
    f32, b16 = jnp.float32, tok_ref.dtype
    nt = (((1,), (1,)), ((), ()))
    nn = (((1,), (0,)), ((), ()))
    y_peer = (2 * z + 1 - y, h)
    x_peer = (e, 2 * (1 - x) + c)
    c_peer = (e, 2 * x + 1 - c)

    eye = (
        lax.broadcasted_iota(jnp.int32, (top, top), 0)
        == lax.broadcasted_iota(jnp.int32, (top, top), 1)
    ).astype(f32)
    flip = lambda a: lax.dot_general(eye, a, nt, preferred_element_type=f32)
    route_t = flip(route_ref[...].astype(f32))
    prob_t = flip(prob_ref[...].astype(f32))
    row_of = lax.broadcasted_iota(jnp.int32, (experts, rows), 0).astype(f32)
    table = jnp.zeros((experts, rows), f32)
    for k in range(top):
        table = table + jnp.where(row_of == route_t[k:k + 1, :], prob_t[k:k + 1, :], 0.0)
    tab_own[...] = table
    tab_in[0, 0] = table

    greet([
        (lax.rem(e + i, groups), lax.rem(h + j, halves))
        for i in range(groups) for j in range(halves) if i + j
    ])
    sends, owns = [], []

    def push(src, dst, peer, number, sem):
        copy = pltpu.make_async_remote_copy(
            src_ref=src, dst_ref=dst, send_sem=number, recv_sem=sem,
            device_id=peer, device_id_type=MESH,
        )
        copy.start()
        sends.append(copy)
        return copy

    def arrived(dst, sem):
        pltpu.make_async_remote_copy(
            src_ref=dst, dst_ref=dst, send_sem=own_sem.at[0], recv_sem=sem,
            device_id=c_peer, device_id_type=MESH,
        ).wait_recv()

    def local(src, dst, sem):
        copy = pltpu.make_async_copy(src, dst, sem)
        copy.start()
        return copy

    def slot(out, s, yy, xx, cc):
        row = pl.multiple_of((2 * s + yy) * rows, rows)
        col = pl.multiple_of((2 * xx + cc) * quarter, quarter)
        return out.at[pl.ds(row, rows), pl.ds(col, quarter)]

    pair = ((tok_ref, xb), (cot_ref, db))

    def at(a, s, kind, cc):
        along = (kind % 2, kind // 2) if a == 0 else (kind // 2, kind % 2)
        return slot(pair[a][1], s, 1 - y if along[0] else y, 1 - x if along[1] else x, cc)

    hops = ((y_peer, x_peer), (x_peer, y_peer))

    def gather_own(s):
        have = []
        for a in range(2):
            there = at(a, s, 0, c)
            if s > 0:
                arrived(there, z_sem.at[a, s])
            have.append((pair[a][0] if s == 0 else there, there))
            push(*have[a], hops[a][0], first_send.at[a, s], p_sem.at[a, s])
        for a in range(2):
            push(*have[a], hops[a][1], second_send.at[a, s], q_sem.at[a, s])
        for a in range(2):
            push(*have[a], c_peer, core_send.at[a, s], c_sem.at[a, s])

    def gather_first(s):
        for a in range(2):
            there = at(a, s, 1, c)
            arrived(there, p_sem.at[a, s])
            push(there, there, hops[a][1], second_send.at[a, line + s], q_sem.at[a, line + s])
        for a in range(2):
            there = at(a, s, 1, c)
            push(there, there, c_peer, core_send.at[a, line + s], c_sem.at[a, line + s])

    def gather_second(s, kind):
        for a in range(2):
            there = at(a, s, kind, c)
            arrived(there, q_sem.at[a, (kind - 2) * line + s])
            push(there, there, c_peer, core_send.at[a, kind * line + s], c_sem.at[a, kind * line + s])

    def gather_core(s):
        for a in range(2):
            for kind in range(4):
                arrived(at(a, s, kind, 1 - c), c_sem.at[a, kind * line + s])

    def plane(s):
        return pl.ds(2 * s * rows, 2 * rows)

    def forward(s):
        gates[...] = lax.dot_general(wgu[...], xb[plane(s), :], nt, preferred_element_type=f32)

    def middle(s):
        raws[...] = lax.dot_general(wdn[...], db[plane(s), :], nt, preferred_element_type=f32)
        chunk = 32 if units % 32 == 0 else 16
        expert_of = lax.broadcasted_iota(jnp.int32, (experts, rows), 0)
        lane = pl.ds(2 * s * rows, 2 * rows)
        sums = []
        tabs = [tab_in[s, y], tab_in[s, 1 - y]]
        for l in range(local_exp):
            weight = jnp.concatenate([
                jnp.sum(jnp.where(expert_of == local_exp * e + l, t, 0.0), axis=0, keepdims=True)
                for t in tabs
            ], axis=1)

            def step(i, total, l=l, weight=weight):
                at_row = pl.multiple_of(l * units + i * chunk, chunk)
                up_row = pl.multiple_of(hidden_rows + l * units + i * chunk, chunk)
                g = gates[pl.ds(at_row, chunk), :]
                u = gates[pl.ds(up_row, chunk), :]
                r = raws[pl.ds(at_row, chunk), :]
                sig = jax.nn.sigmoid(g)
                act = g * sig
                hidden = act * u
                dact = weight * r
                hps[pl.ds(at_row, chunk), lane] = (weight * hidden).astype(b16)
                dgu[pl.ds(at_row, chunk), lane] = (
                    dact * u * sig * (1.0 + g * (1.0 - sig))
                ).astype(b16)
                dgu[pl.ds(up_row, chunk), lane] = (dact * act).astype(b16)
                return total + jnp.sum((hidden * r).reshape(chunk // 8, 8, 2 * rows), axis=0)

            total = lax.fori_loop(0, units // chunk, step, jnp.zeros((8, 2 * rows), f32))
            sums.append(jnp.sum(total, axis=0, keepdims=True))
        sub = lax.broadcasted_iota(jnp.int32, (8, rows), 0)
        for yy in range(2):
            block = jnp.zeros((8, rows), f32)
            for l in range(local_exp):
                block = jnp.where(sub == l, sums[l][:, yy * rows:(yy + 1) * rows], block)
            score[s, yy] = block
        turned[...] = dgu[:, lane].T

    def part_of(xx, cc):
        cols = pl.ds(pl.multiple_of((2 * xx + cc) * quarter, quarter), quarter)
        return lax.dot_general(turned[...], wgu[:, cols], nn, preferred_element_type=f32).astype(b16)

    def send_part(s):
        copies = []
        for xx in range(2):
            psend[s, xx] = part_of(xx, 1 - c)
        for xx in range(2):
            push(psend.at[s, xx], cin.at[s, xx], c_peer, part_send.at[s, xx], part_recv.at[s, xx])
        for xx in range(2):
            own[s, xx] = part_of(xx, c)

    def flipped(dy):
        return 1 - y if dy else y

    def send_score(s):
        for dy in range(2):
            for j in range(halves):
                if s + dy + j == 0:
                    owns.append(local(score.at[0, y], back.at[0, 0, h], own_sem.at[3]))
                    continue
                push(
                    score.at[s, flipped(dy)], back.at[s, dy, h],
                    (2 * across(z, s) + flipped(dy), lax.rem(h + j, halves)),
                    score_send.at[s, dy, j], score_recv.at[s, dy, j],
                )

    step_rows = 32

    def row_loop(count):
        return pl.loop(0, count // step_rows)

    def some(i):
        return pl.ds(pl.multiple_of(i * step_rows, step_rows), step_rows)

    def settle_core(s):
        for xx in range(2):
            arrived(cin.at[s, xx], part_recv.at[s, xx])

            @row_loop(2 * rows)
            def _(i):
                both = own[s, xx, some(i)].astype(f32) + cin[s, xx, some(i)].astype(f32)
                acc[s, 0, xx, some(i)] = both[:, :wide].astype(b16)
                acc[s, 1, xx, some(i)] = both[:, wide:].astype(b16)

        push(acc.at[s, 0, 1 - x], xin0.at[s], x_peer, hop_send.at[s, 0], hop_recv.at[s, 0])
        away = pl.ds(pl.multiple_of((1 - y) * rows, rows), rows)
        push(acc.at[s, 1, :, away], yin1.at[s], y_peer, hop_send.at[s, 1], hop_recv.at[s, 1])

    def settle_first(s):
        arrived(xin0.at[s], hop_recv.at[s, 0])

        @row_loop(2 * rows)
        def _(i):
            t0[s, some(i)] = (
                acc[s, 0, x, some(i)].astype(f32) + xin0[s, some(i)].astype(f32)
            ).astype(b16)

        away = pl.ds(pl.multiple_of((1 - y) * rows, rows), rows)
        push(t0.at[s, away], yin0.at[s], y_peer, hop_send.at[s, 2], hop_recv.at[s, 2])
        arrived(yin1.at[s], hop_recv.at[s, 1])

        @row_loop(rows)
        def _(i):
            here = pl.ds(pl.multiple_of(y * rows + i * step_rows, step_rows), step_rows)
            for xx in range(2):
                t1[s, xx, some(i)] = (
                    acc[s, 1, xx, here].astype(f32) + yin1[s, xx, some(i)].astype(f32)
                ).astype(b16)

        push(t1.at[s, 1 - x], xin1.at[s], x_peer, hop_send.at[s, 3], hop_recv.at[s, 3])

    def settle_second(s):
        arrived(yin0.at[s], hop_recv.at[s, 2])
        arrived(xin1.at[s], hop_recv.at[s, 3])

        @row_loop(rows)
        def _(i):
            here = pl.ds(pl.multiple_of(y * rows + i * step_rows, step_rows), step_rows)
            fin[s, some(i), :wide] = (
                t0[s, here].astype(f32) + yin0[s, some(i)].astype(f32)
            ).astype(b16)
            fin[s, some(i), wide:] = (
                t1[s, x, some(i)].astype(f32) + xin1[s, some(i)].astype(f32)
            ).astype(b16)

        if s > 0:
            push(fin.at[s], zin.at[s], (2 * across(z, s) + y, h), last_send.at[s], last_recv.at[s])

    cut = quarter

    def grads_in(n):
        cols = pl.ds(n * cut, cut)
        both = lax.dot_general(dgu[...], xb[:, cols], nn, preferred_element_type=f32).astype(b16)
        gg_ref[:, cols] = both[:hidden_rows]
        gu_ref[:, cols] = both[hidden_rows:]

    def grads_out(n):
        cols = pl.ds(n * cut, cut)
        gd_ref[:, cols] = lax.dot_general(
            hps[...], db[:, cols], nn, preferred_element_type=f32
        ).astype(b16)

    gather_own(0)
    for a in range(2):
        for s in range(1, line):
            push(
                pair[a][0], slot(pair[a][1], s, y, x, c), (2 * across(z, s) + y, h),
                z_send.at[a, s], z_sem.at[a, s],
            )
    weights = [
        local(wg_ref, wgu.at[pl.ds(0, hidden_rows)], w_sem.at[0]),
        local(wu_ref, wgu.at[pl.ds(hidden_rows, hidden_rows)], w_sem.at[1]),
        local(wd_ref, wdn, w_sem.at[2]),
    ]
    mine = [local(pair[a][0], at(a, 0, 0, c), own_sem.at[1 + a]) for a in range(2)]
    for s in range(line):
        for dy in range(2):
            if s + dy:
                push(
                    tab_own, tab_in.at[s, dy], (2 * across(z, s) + flipped(dy), h),
                    tab_send.at[s, dy], tab_recv.at[s, dy],
                )
    gather_first(0)
    for copy in weights + mine:
        copy.wait()

    for s in range(line):
        if s + 1 < line:
            gather_own(s + 1)
        if s >= 1:
            settle_core(s - 1)
        gather_second(s, 2)
        gather_second(s, 3)
        gather_core(s)
        for dy in range(2):
            if s + dy:
                arrived(tab_in.at[s, dy], tab_recv.at[s, dy])
        if s >= 2:
            settle_second(s - 2)
        forward(s)
        if s + 1 < line:
            gather_first(s + 1)
        if s >= 1:
            settle_first(s - 1)
        middle(s)
        send_part(s)
        send_score(s)

    settle_core(line - 1)
    settle_second(line - 2)
    pieces = width // cut
    halfway = pieces // 2
    for n in range(halfway):
        grads_in(n)
    settle_first(line - 1)
    for n in range(halfway, pieces):
        grads_in(n)
    settle_second(line - 1)
    for n in range(pieces):
        grads_out(n)

    for copy in owns:
        copy.wait()
    for s in range(line):
        for dy in range(2):
            for j in range(halves):
                if s + dy + j:
                    arrived(
                        back.at[s, dy, lax.rem(h + halves - j, halves)], score_recv.at[s, dy, j]
                    )
    total = jnp.zeros((top, rows), f32)
    for s in range(line):
        for dy in range(2):
            block = back[s, dy, 0]
            for j in range(1, halves):
                block = block + back[s, dy, j]
            first = local_exp * (2 * across(z, s) + flipped(dy))
            for l in range(local_exp):
                total = total + jnp.where(
                    route_t == (first + l).astype(f32), block[l:l + 1, :], 0.0
                )
    gp_ref[...] = total
    for s in range(1, line):
        arrived(zin.at[s], last_recv.at[s])

    @row_loop(rows)
    def _(i):
        whole = fin[0, some(i)].astype(f32)
        for s in range(1, line):
            whole = whole + zin[s, some(i)].astype(f32)
        gt_ref[some(i)] = whole.astype(b16)

    for copy in sends:
        copy.wait_send()


def fused(tokens, cotangent, route, prob, wg, wu, wd, groups, halves, local_exp):
    rows, quarter = tokens.shape
    line, wide = groups // 2, quarter // 2
    hidden_rows, width = wg.shape
    experts, top = local_exp * groups, route.shape[1]
    b16, f32 = tokens.dtype, jnp.float32
    dma = pltpu.SemaphoreType.DMA
    vmem = pl.BlockSpec(memory_space=pltpu.VMEM)
    hbm = pl.BlockSpec(memory_space=pl.ANY)
    total = groups * rows
    grad = jax.ShapeDtypeStruct((hidden_rows, width), b16)
    return pl.pallas_call(
        functools.partial(fused_kernel, groups, halves, local_exp),
        out_shape=(
            jax.ShapeDtypeStruct((rows, quarter), b16),
            jax.ShapeDtypeStruct((top, rows), f32),
            grad, grad, grad,
        ),
        in_specs=[vmem] * 4 + [hbm] * 3,
        out_specs=[vmem] * 5,
        scratch_shapes=[
            pltpu.VMEM((total, width), b16),
            pltpu.VMEM((total, width), b16),
            pltpu.VMEM((2 * hidden_rows, width), b16),
            pltpu.VMEM((hidden_rows, width), b16),
            pltpu.VMEM((2 * hidden_rows, 2 * rows), f32),
            pltpu.VMEM((hidden_rows, 2 * rows), f32),
            pltpu.VMEM((2 * hidden_rows, total), b16),
            pltpu.VMEM((hidden_rows, total), b16),
            pltpu.VMEM((2 * rows, 2 * hidden_rows), b16),
            pltpu.VMEM((experts, rows), f32),
            pltpu.VMEM((line, 2, experts, rows), f32),
            pltpu.VMEM((line, 2, 8, rows), f32),
            pltpu.VMEM((line, 2, halves, 8, rows), f32),
            pltpu.VMEM((line, 2, 2 * rows, quarter), b16),
            pltpu.VMEM((line, 2, 2 * rows, quarter), b16),
            pltpu.VMEM((line, 2, 2 * rows, quarter), b16),
            pltpu.VMEM((line, 2, 2, 2 * rows, wide), b16),
            pltpu.VMEM((line, 2 * rows, wide), b16),
            pltpu.VMEM((line, rows, wide), b16),
            pltpu.VMEM((line, 2, rows, wide), b16),
            pltpu.VMEM((line, rows, wide), b16),
            pltpu.VMEM((line, 2 * rows, wide), b16),
            pltpu.VMEM((line, 2, rows, wide), b16),
            pltpu.VMEM((line, rows, quarter), b16),
            pltpu.VMEM((line, rows, quarter), b16),
            dma((2, line)), dma((2, 2 * line)), dma((2, 4 * line)), dma((2, line)),
            dma((2, line)), dma((2, line)), dma((2, 2 * line)), dma((2, 4 * line)),
            dma((4,)), dma((3,)),
            dma((line, 2)), dma((line, 2)),
            dma((line, 2, halves)), dma((line, 2, halves)),
            dma((line, 2)), dma((line, 2)),
            dma((line, 4)), dma((line, 4)),
            dma((line,)), dma((line,)),
        ],
        compiler_params=pltpu.CompilerParams(
            collective_id=0, has_side_effects=True, vmem_limit_bytes=VMEM_BYTES
        ),
    )(tokens, cotangent, route, prob, wg, wu, wd)


def per_device(tokens, cotangent, route, prob, w_gate, w_up, w_down):
    tok_rows, quarter = tokens.shape
    local_exp, units, width = w_gate.shape
    groups = lax.axis_size("expert")
    halves = lax.axis_size("half")
    experts = local_exp * groups
    total = groups * tok_rows
    f32 = jnp.float32
    me = lax.axis_index("expert")

    fast = (
        groups > 2 and groups & (groups - 1) == 0 and halves == 2 * 2
        and tok_rows == LANES and quarter % (2 * LANES) == 0
        and units % 16 == 0 and local_exp <= 8 and experts <= 2 * LANES and route.shape[1] <= 8
        and 2 * total * width * 2 + 12 * local_exp * units * width <= VMEM_BYTES // 2
    )
    if fast:
        flat = (local_exp * units, width)
        grad_tokens, grad_prob, *grads = fused(
            tokens, cotangent, route, prob, w_gate.reshape(flat), w_up.reshape(flat),
            w_down.reshape(flat), groups, halves, local_exp,
        )
        grads = [g.reshape(local_exp, units, width) for g in grads]
        return (grad_tokens, grad_prob.T, *grads)

    hit = route[:, :, None] == jnp.arange(experts, dtype=route.dtype)
    table = jnp.sum(jnp.where(hit, prob[:, :, None], 0).astype(f32), axis=1).astype(prob.dtype)
    mine = lax.all_to_all(
        table.reshape(tok_rows, groups, local_exp), "expert",
        split_axis=1, concat_axis=0, tiled=True,
    ).reshape(total, local_exp)
    x = gather_all(tokens, groups, halves)
    d = gather_all(cotangent, groups, halves)
    weight = jnp.repeat(mine.astype(f32), units, axis=1)

    wg = w_gate.reshape(local_exp * units, width)
    wu = w_up.reshape(local_exp * units, width)
    wd = w_down.reshape(local_exp * units, width)
    nt = (((1,), (1,)), ((), ()))
    tn = (((0,), (0,)), ((), ()))
    gate = lax.dot_general(x, wg, nt, preferred_element_type=f32)
    upval = lax.dot_general(x, wu, nt, preferred_element_type=f32)
    raw = lax.dot_general(d, wd, nt, preferred_element_type=f32)
    sig = jax.nn.sigmoid(gate)
    act = gate * sig
    hidden = act * upval
    score = jnp.sum((hidden * raw).reshape(total, local_exp, units), axis=2)
    dact = weight * raw
    hp = (weight * hidden).astype(jnp.bfloat16)
    dgate = (dact * upval * sig * (1.0 + gate * (1.0 - sig))).astype(jnp.bfloat16)
    dup = (dact * act).astype(jnp.bfloat16)
    part = lax.dot_general(
        jnp.concatenate([dgate, dup], axis=1), jnp.concatenate([wg, wu], axis=0),
        (((1,), (0,)), ((), ())), preferred_element_type=f32,
    ).astype(jnp.bfloat16)
    part = part.reshape(groups, tok_rows, halves, quarter).transpose(0, 2, 1, 3)
    grad_tokens = lax.psum_scatter(
        part.reshape(groups * halves * tok_rows, quarter), BOTH,
        scatter_dimension=0, tiled=True,
    )
    sent = jnp.broadcast_to(
        score.reshape(groups, 1, tok_rows, local_exp), (groups, halves, tok_rows, local_exp)
    ).reshape(groups * halves, tok_rows * local_exp)
    back = lax.all_to_all(sent, BOTH, split_axis=0, concat_axis=0, tiled=True)
    back = jnp.sum(back.reshape(groups, halves, tok_rows, local_exp), axis=1)
    back = back.transpose(1, 0, 2).reshape(tok_rows, 1, experts)
    grad_prob = jnp.sum(jnp.where(hit, back, 0), axis=2)
    shape = (local_exp, units, width)
    grad_gate = lax.dot_general(dgate, x, tn, preferred_element_type=f32).astype(jnp.bfloat16)
    grad_up = lax.dot_general(dup, x, tn, preferred_element_type=f32).astype(jnp.bfloat16)
    grad_down = lax.dot_general(hp, d, tn, preferred_element_type=f32).astype(jnp.bfloat16)
    return (
        grad_tokens,
        grad_prob,
        grad_gate.reshape(shape),
        grad_up.reshape(shape),
        grad_down.reshape(shape),
    )


def solution(mesh):
    in_specs = (
        P("expert", "half"),
        P("expert", "half"),
        P("expert", None),
        P("expert", None),
        P("expert", "half", None),
        P("expert", "half", None),
        P("expert", "half", None),
    )
    out_specs = (
        P("expert", "half"),
        P("expert", None),
        P("expert", "half", None),
        P("expert", "half", None),
        P("expert", "half", None),
    )
    return jax.shard_map(
        per_device, mesh=mesh, in_specs=in_specs, out_specs=out_specs, check_vma=False
    )
```

```python
import functools

import jax
import jax.numpy as jnp
from jax import lax
from jax.experimental import pallas as pl
from jax.experimental.pallas import tpu as pltpu
from jax.sharding import PartitionSpec as P

BOTH = ("expert", "half")


def gather_all(block, groups, halves):
    rows, quarter = block.shape
    parts = lax.all_gather(block, BOTH, axis=0).reshape(groups, halves, rows, quarter)
    return parts.transpose(0, 2, 1, 3).reshape(groups * rows, halves * quarter)


LANES = 128
VMEM_BYTES = 48 << 20
DRAIN_BYTES = 1 << 20
MESH = pl.DeviceIdType.MESH


def place(groups):
    e, h = lax.axis_index("expert"), lax.axis_index("half")
    return lax.div(e, 2), lax.rem(e, 2), lax.div(h, 2), lax.rem(h, 2)


def across(z, step):
    bit = 1
    while bit <= step:
        if step & bit:
            z = z + bit * (1 - 2 * lax.rem(lax.div(z, bit), 2))
        bit *= 2
    return z


def greet(peers):
    barrier = pltpu.get_barrier_semaphore()
    for peer in peers:
        pl.semaphore_signal(barrier, inc=1, device_id=peer, device_id_type=MESH)
    pl.semaphore_wait(barrier, len(peers))


def fused_kernel(
    groups, halves, local_exp, tok_ref, cot_ref, route_ref, prob_ref, wg_ref, wu_ref, wd_ref,
    gt_ref, gp_ref, gg_ref, gu_ref, gd_ref,
    xb, db, wgu, wdn, gates, raws, dgu, hps, turned, route_in, prob_in, tab_own, tab_in, score, back,
    psend, own, cin, acc, xin0, yin0, yin1, xin1, t0, t1, fin, zin,
    first_send, second_send, core_send, rest_send, z_send, z_sem, p_sem, q_sem, c_sem, own_sem, w_sem,
    tab_send, tab_recv, score_send, score_recv,
    part_send, part_recv, hop_send, hop_recv, last_send, last_recv,
):
    line = groups // 2
    z, y, x, c = place(groups)
    e, h = 2 * z + y, 2 * x + c
    rows, quarter = tok_ref.shape
    wide = quarter // 2
    hidden_rows, width = wg_ref.shape
    units = hidden_rows // local_exp
    experts = local_exp * groups
    top = route_ref.shape[0]
    f32, b16 = jnp.float32, tok_ref.dtype
    nt = (((1,), (1,)), ((), ()))
    nn = (((1,), (0,)), ((), ()))
    y_peer = (2 * z + 1 - y, h)
    x_peer = (e, 2 * (1 - x) + c)
    c_peer = (e, 2 * x + 1 - c)

    def local(src, dst, sem):
        copy = pltpu.make_async_copy(src, dst, sem)
        copy.start()
        return copy

    def slot(out, s, yy, xx, cc):
        row = pl.multiple_of((2 * s + yy) * rows, rows)
        col = pl.multiple_of((2 * xx + cc) * quarter, quarter)
        return out.at[pl.ds(row, rows), pl.ds(col, quarter)]

    pair = ((tok_ref, xb), (cot_ref, db))

    def at(a, s, kind, cc):
        over = (kind % 2, kind // 2) if a == 0 else (kind // 2, kind % 2)
        return slot(pair[a][1], s, 1 - y if over[0] else y, 1 - x if over[1] else x, cc)

    mine = [local(pair[a][0], at(a, 0, 0, c), own_sem.at[1 + a]) for a in range(2)]

    small = [local(route_ref, route_in, w_sem.at[3]), local(prob_ref, prob_in, w_sem.at[4])]
    for copy in small:
        copy.wait()
    route_t = route_in[...]
    prob_t = prob_in[...].astype(f32)
    row_of = lax.broadcasted_iota(jnp.int32, (experts, rows), 0)
    table = jnp.zeros((experts, rows), f32)
    for k in range(top):
        table = table + jnp.where(row_of == route_t[k:k + 1, :], prob_t[k:k + 1, :], 0.0)
    tab_own[...] = table
    tab_in[0, 0] = table

    greet([
        (lax.rem(e + i, groups), lax.rem(h + j, halves))
        for i in range(groups) for j in range(halves) if i + j
    ])
    sends, owns = [], []

    def push(src, dst, peer, number, sem):
        copy = pltpu.make_async_remote_copy(
            src_ref=src, dst_ref=dst, send_sem=number, recv_sem=sem,
            device_id=peer, device_id_type=MESH,
        )
        copy.start()
        sends.append(copy)
        return copy

    def arrived(dst, sem):
        pltpu.make_async_remote_copy(
            src_ref=dst, dst_ref=dst, send_sem=own_sem.at[0], recv_sem=sem,
            device_id=c_peer, device_id_type=MESH,
        ).wait_recv()

    hops = ((y_peer, x_peer), (x_peer, y_peer))

    def gather_own(s):
        have = [at(a, s, 0, c) for a in range(2)]
        for a in range(2):
            if s > 0:
                arrived(have[a], z_sem.at[a, s])
            if s != 1:
                push(have[a], have[a], hops[a][0], first_send.at[a, s], p_sem.at[a, s])
        for a in range(2):
            push(have[a], have[a], hops[a][1], second_send.at[a, s], q_sem.at[a, s])
        for a in range(2):
            push(have[a], have[a], c_peer, core_send.at[a, s], c_sem.at[a, s])

    def gather_first(s):
        there = [at(a, s, 1, c) for a in range(2)]
        for a in range(2):
            arrived(there[a], p_sem.at[a, s])
            if s != 1:
                push(
                    there[a], there[a], hops[a][1],
                    second_send.at[a, line + s], q_sem.at[a, line + s],
                )
        for a in range(2):
            push(there[a], there[a], c_peer, core_send.at[a, line + s], c_sem.at[a, line + s])

    def gather_second(s, kind):
        for a in range(2):
            there = at(a, s, kind, c)
            arrived(there, q_sem.at[a, (kind - 2) * line + s])
            push(there, there, c_peer, core_send.at[a, kind * line + s], c_sem.at[a, kind * line + s])

    def along(s):
        return (2 * across(z, s) + y, h)

    def send_plane(s):
        for a in range(2):
            push(at(a, 0, 0, c), at(a, s, 0, c), along(s), z_send.at[a, s], z_sem.at[a, s])

    def send_rest(kind):
        for a in range(2):
            sem = p_sem.at[a, 1] if kind == 1 else q_sem.at[a, line + 1]
            push(at(a, 0, kind, c), at(a, 1, kind, c), along(1), rest_send.at[a, kind // 2], sem)

    def gather_core(s):
        for a in range(2):
            for kind in range(4):
                arrived(at(a, s, kind, 1 - c), c_sem.at[a, kind * line + s])

    def plane(s):
        return pl.ds(2 * s * rows, 2 * rows)

    def forward(s):
        gates[...] = lax.dot_general(wgu[...], xb[plane(s), :], nt, preferred_element_type=f32)

    def middle(s):
        raws[...] = lax.dot_general(wdn[...], db[plane(s), :], nt, preferred_element_type=f32)
        chunk = 32 if units % 32 == 0 else 16
        expert_of = lax.broadcasted_iota(jnp.int32, (experts, rows), 0)
        lane = pl.ds(2 * s * rows, 2 * rows)
        sums = []
        tabs = [tab_in[s, y], tab_in[s, 1 - y]]
        for l in range(local_exp):
            weight = jnp.concatenate([
                jnp.sum(jnp.where(expert_of == local_exp * e + l, t, 0.0), axis=0, keepdims=True)
                for t in tabs
            ], axis=1)

            def step(i, total, l=l, weight=weight):
                at_row = pl.multiple_of(l * units + i * chunk, chunk)
                up_row = pl.multiple_of(hidden_rows + l * units + i * chunk, chunk)
                g = gates[pl.ds(at_row, chunk), :]
                u = gates[pl.ds(up_row, chunk), :]
                r = raws[pl.ds(at_row, chunk), :]
                sig = jax.nn.sigmoid(g)
                act = g * sig
                hidden = act * u
                dact = weight * r
                hps[pl.ds(at_row, chunk), lane] = (weight * hidden).astype(b16)
                dgu[pl.ds(at_row, chunk), lane] = (
                    dact * u * sig * (1.0 + g * (1.0 - sig))
                ).astype(b16)
                dgu[pl.ds(up_row, chunk), lane] = (dact * act).astype(b16)
                return total + jnp.sum((hidden * r).reshape(chunk // 8, 8, 2 * rows), axis=0)

            total = lax.fori_loop(0, units // chunk, step, jnp.zeros((8, 2 * rows), f32))
            sums.append(jnp.sum(total, axis=0, keepdims=True))
        sub = lax.broadcasted_iota(jnp.int32, (8, rows), 0)
        for yy in range(2):
            block = jnp.zeros((8, rows), f32)
            for l in range(local_exp):
                block = jnp.where(sub == l, sums[l][:, yy * rows:(yy + 1) * rows], block)
            score[s, yy] = block
        turned[...] = dgu[:, lane].T

    def part_of(xx, cc):
        cols = pl.ds(pl.multiple_of((2 * xx + cc) * quarter, quarter), quarter)
        return lax.dot_general(turned[...], wgu[:, cols], nn, preferred_element_type=f32).astype(b16)

    def send_part(s):
        copies = []
        for xx in range(2):
            psend[s, xx] = part_of(xx, 1 - c)
            push(psend.at[s, xx], cin.at[s, xx], c_peer, part_send.at[s, xx], part_recv.at[s, xx])
        for xx in range(2):
            own[s, xx] = part_of(xx, c)

    def flipped(dy):
        return 1 - y if dy else y

    def send_score(s):
        for dy in range(2):
            for j in range(halves):
                if s + dy + j == 0:
                    owns.append(local(score.at[0, y], back.at[0, 0, h], own_sem.at[3]))
                    continue
                push(
                    score.at[s, flipped(dy)], back.at[s, dy, h],
                    (2 * across(z, s) + flipped(dy), lax.rem(h + j, halves)),
                    score_send.at[s, dy, j], score_recv.at[s, dy, j],
                )

    step_rows = 32

    def row_loop(count):
        return pl.loop(0, count // step_rows)

    def some(i):
        return pl.ds(pl.multiple_of(i * step_rows, step_rows), step_rows)

    def settle_core(s):
        for xx in range(2):
            arrived(cin.at[s, xx], part_recv.at[s, xx])

            @row_loop(2 * rows)
            def _(i):
                both = own[s, xx, some(i)].astype(f32) + cin[s, xx, some(i)].astype(f32)
                acc[s, 0, xx, some(i)] = both[:, :wide].astype(b16)
                acc[s, 1, xx, some(i)] = both[:, wide:].astype(b16)

        push(acc.at[s, 0, 1 - x], xin0.at[s], x_peer, hop_send.at[s, 0], hop_recv.at[s, 0])
        away = pl.ds(pl.multiple_of((1 - y) * rows, rows), rows)
        push(acc.at[s, 1, :, away], yin1.at[s], y_peer, hop_send.at[s, 1], hop_recv.at[s, 1])

    def settle_first(s):
        arrived(xin0.at[s], hop_recv.at[s, 0])

        @row_loop(2 * rows)
        def _(i):
            t0[s, some(i)] = (
                acc[s, 0, x, some(i)].astype(f32) + xin0[s, some(i)].astype(f32)
            ).astype(b16)

        away = pl.ds(pl.multiple_of((1 - y) * rows, rows), rows)
        push(t0.at[s, away], yin0.at[s], y_peer, hop_send.at[s, 2], hop_recv.at[s, 2])
        arrived(yin1.at[s], hop_recv.at[s, 1])

        @row_loop(rows)
        def _(i):
            here = pl.ds(pl.multiple_of(y * rows + i * step_rows, step_rows), step_rows)
            for xx in range(2):
                t1[s, xx, some(i)] = (
                    acc[s, 1, xx, here].astype(f32) + yin1[s, xx, some(i)].astype(f32)
                ).astype(b16)

        push(t1.at[s, 1 - x], xin1.at[s], x_peer, hop_send.at[s, 3], hop_recv.at[s, 3])

    def settle_second(s):
        arrived(yin0.at[s], hop_recv.at[s, 2])
        arrived(xin1.at[s], hop_recv.at[s, 3])

        @row_loop(rows)
        def _(i):
            here = pl.ds(pl.multiple_of(y * rows + i * step_rows, step_rows), step_rows)
            fin[s, some(i), :wide] = (
                t0[s, here].astype(f32) + yin0[s, some(i)].astype(f32)
            ).astype(b16)
            fin[s, some(i), wide:] = (
                t1[s, x, some(i)].astype(f32) + xin1[s, some(i)].astype(f32)
            ).astype(b16)

        if s > 0:
            push(fin.at[s], zin.at[s], (2 * across(z, s) + y, h), last_send.at[s], last_recv.at[s])

    cut = quarter

    def grads_in(n):
        cols = pl.ds(n * cut, cut)
        both = lax.dot_general(dgu[...], xb[:, cols], nn, preferred_element_type=f32).astype(b16)
        gg_ref[:, cols] = both[:hidden_rows]
        gu_ref[:, cols] = both[hidden_rows:]

    def grads_out(n):
        cols = pl.ds(n * cut, cut)
        gd_ref[:, cols] = lax.dot_general(
            hps[...], db[:, cols], nn, preferred_element_type=f32
        ).astype(b16)

    for copy in mine:
        copy.wait()
    def send_table():
        for s in range(line):
            for dy in range(2):
                if s + dy:
                    push(
                        tab_own, tab_in.at[s, dy], (2 * across(z, s) + flipped(dy), h),
                        tab_send.at[s, dy], tab_recv.at[s, dy],
                    )

    def table_in(s):
        for dy in range(2):
            if s + dy:
                arrived(tab_in.at[s, dy], tab_recv.at[s, dy])

    def finish(s):
        middle(s)
        send_part(s)
        send_score(s)

    gather_own(0)
    send_plane(1)
    send_plane(2)
    send_table()
    weights = [
        local(wg_ref, wgu.at[pl.ds(0, hidden_rows)], w_sem.at[0]),
        local(wu_ref, wgu.at[pl.ds(hidden_rows, hidden_rows)], w_sem.at[1]),
        local(wd_ref, wdn, w_sem.at[2]),
    ]
    gather_first(0)
    gather_second(0, 2)
    gather_own(1)
    send_plane(3)
    send_rest(1)
    gather_second(0, 3)
    send_rest(3)
    gather_core(0)
    for copy in weights:
        copy.wait()
    table_in(0)
    forward(0)
    gather_own(2)
    finish(0)
    gather_second(1, 2)
    gather_first(2)
    settle_core(0)
    gather_second(2, 2)
    gather_second(2, 3)
    gather_core(2)
    table_in(2)
    forward(2)
    gather_own(3)
    finish(2)
    settle_first(0)
    gather_first(3)
    settle_core(2)
    gather_first(1)
    gather_second(1, 3)
    gather_core(1)
    table_in(1)
    forward(1)
    finish(1)
    settle_second(0)
    gather_second(3, 2)
    gather_second(3, 3)
    gather_core(3)
    settle_core(1)
    table_in(3)
    forward(3)
    settle_first(2)
    finish(3)
    settle_second(2)
    settle_first(1)
    settle_core(3)
    grads_in(0)
    grads_in(1)
    settle_second(1)
    settle_first(3)
    grads_in(2)
    grads_in(3)
    settle_second(3)
    for n in range(width // cut):
        grads_out(n)

    for copy in owns:
        copy.wait()
    for s in range(line):
        for dy in range(2):
            for j in range(halves):
                if s + dy + j:
                    arrived(
                        back.at[s, dy, lax.rem(h + halves - j, halves)], score_recv.at[s, dy, j]
                    )
    total = jnp.zeros((top, rows), f32)
    for s in range(line):
        for dy in range(2):
            block = back[s, dy, 0]
            for j in range(1, halves):
                block = block + back[s, dy, j]
            first = local_exp * (2 * across(z, s) + flipped(dy))
            for l in range(local_exp):
                total = total + jnp.where(
                    route_t == first + l, block[l:l + 1, :], 0.0
                )
    gp_ref[...] = total
    for s in range(1, line):
        arrived(zin.at[s], last_recv.at[s])

    @row_loop(rows)
    def _(i):
        whole = fin[0, some(i)].astype(f32)
        for s in range(1, line):
            whole = whole + zin[s, some(i)].astype(f32)
        gt_ref[some(i)] = whole.astype(b16)

    for copy in sends:
        copy.wait_send()


def fused(tokens, cotangent, route, prob, wg, wu, wd, groups, halves, local_exp):
    rows, quarter = tokens.shape
    line, wide = groups // 2, quarter // 2
    hidden_rows, width = wg.shape
    experts, top = local_exp * groups, route.shape[0]
    b16, f32 = tokens.dtype, jnp.float32
    dma = pltpu.SemaphoreType.DMA
    vmem = pl.BlockSpec(memory_space=pltpu.VMEM)
    hbm = pl.BlockSpec(memory_space=pltpu.HBM)
    total = groups * rows
    grad = jax.ShapeDtypeStruct((hidden_rows, width), b16)
    return pl.pallas_call(
        functools.partial(fused_kernel, groups, halves, local_exp),
        out_shape=(
            jax.ShapeDtypeStruct((rows, quarter), b16),
            jax.ShapeDtypeStruct((top, rows), f32),
            grad, grad, grad,
        ),
        in_specs=[hbm] * 7,
        out_specs=[vmem] * 5,
        scratch_shapes=[
            pltpu.VMEM((total, width), b16),
            pltpu.VMEM((total, width), b16),
            pltpu.VMEM((2 * hidden_rows, width), b16),
            pltpu.VMEM((hidden_rows, width), b16),
            pltpu.VMEM((2 * hidden_rows, 2 * rows), f32),
            pltpu.VMEM((hidden_rows, 2 * rows), f32),
            pltpu.VMEM((2 * hidden_rows, total), b16),
            pltpu.VMEM((hidden_rows, total), b16),
            pltpu.VMEM((2 * rows, 2 * hidden_rows), b16),
            pltpu.VMEM(route.shape, route.dtype),
            pltpu.VMEM(prob.shape, prob.dtype),
            pltpu.VMEM((experts, rows), f32),
            pltpu.VMEM((line, 2, experts, rows), f32),
            pltpu.VMEM((line, 2, 8, rows), f32),
            pltpu.VMEM((line, 2, halves, 8, rows), f32),
            pltpu.VMEM((line, 2, 2 * rows, quarter), b16),
            pltpu.VMEM((line, 2, 2 * rows, quarter), b16),
            pltpu.VMEM((line, 2, 2 * rows, quarter), b16),
            pltpu.VMEM((line, 2, 2, 2 * rows, wide), b16),
            pltpu.VMEM((line, 2 * rows, wide), b16),
            pltpu.VMEM((line, rows, wide), b16),
            pltpu.VMEM((line, 2, rows, wide), b16),
            pltpu.VMEM((line, rows, wide), b16),
            pltpu.VMEM((line, 2 * rows, wide), b16),
            pltpu.VMEM((line, 2, rows, wide), b16),
            pltpu.VMEM((line, rows, quarter), b16),
            pltpu.VMEM((line, rows, quarter), b16),
            dma((2, line)), dma((2, 2 * line)), dma((2, 4 * line)), dma((2, 2)), dma((2, line)),
            dma((2, line)), dma((2, line)), dma((2, 2 * line)), dma((2, 4 * line)),
            dma((4,)), dma((5,)),
            dma((line, 2)), dma((line, 2)),
            dma((line, 2, halves)), dma((line, 2, halves)),
            dma((line, 2)), dma((line, 2)),
            dma((line, 4)), dma((line, 4)),
            dma((line,)), dma((line,)),
        ],
        compiler_params=pltpu.CompilerParams(
            collective_id=0, has_side_effects=True, vmem_limit_bytes=VMEM_BYTES
        ),
    )(tokens, cotangent, route, prob, wg, wu, wd)


def drain_kernel(count, *refs):
    sources, targets, sem = refs[:count], refs[count:2 * count], refs[2 * count]
    copies = [pltpu.make_async_copy(a, b, sem.at[i]) for i, (a, b) in enumerate(zip(sources, targets))]
    for copy in copies:
        copy.start()
    for copy in copies:
        copy.wait()


def drain(arrays):
    count = len(arrays)
    return pl.pallas_call(
        functools.partial(drain_kernel, count),
        out_shape=[jax.ShapeDtypeStruct(a.shape, a.dtype) for a in arrays],
        in_specs=[pl.BlockSpec(memory_space=pltpu.VMEM)] * count,
        out_specs=[pl.BlockSpec(memory_space=pl.ANY)] * count,
        scratch_shapes=[pltpu.SemaphoreType.DMA((count,))],
        compiler_params=pltpu.CompilerParams(vmem_limit_bytes=DRAIN_BYTES),
    )(*arrays)


def per_device(tokens, cotangent, route, prob, w_gate, w_up, w_down):
    tok_rows, quarter = tokens.shape
    local_exp, units, width = w_gate.shape
    groups = lax.axis_size("expert")
    halves = lax.axis_size("half")
    experts = local_exp * groups
    total = groups * tok_rows
    f32 = jnp.float32
    me = lax.axis_index("expert")

    fast = (
        groups == 2 * halves and halves == 2 * 2 and width == 4 * quarter
        and tok_rows == LANES and quarter % (2 * LANES) == 0
        and units % 16 == 0 and local_exp <= 8 and experts <= 2 * LANES and route.shape[1] <= 8
        and 2 * total * width * 2 + 12 * local_exp * units * width <= VMEM_BYTES // 2
    )
    if fast:
        flat = (local_exp * units, width)
        results = fused(
            *[pltpu.with_memory_space_constraint(v, pltpu.HBM) for v in (tokens, cotangent, route.T, prob.T)], w_gate.reshape(flat), w_up.reshape(flat),
            w_down.reshape(flat), groups, halves, local_exp,
        )
        grad_tokens, grad_prob, *grads = drain(results)
        grads = [g.reshape(local_exp, units, width) for g in grads]
        return (grad_tokens, grad_prob.T, *grads)

    hit = route[:, :, None] == jnp.arange(experts, dtype=route.dtype)
    table = jnp.sum(jnp.where(hit, prob[:, :, None], 0).astype(f32), axis=1).astype(prob.dtype)
    mine = lax.all_to_all(
        table.reshape(tok_rows, groups, local_exp), "expert",
        split_axis=1, concat_axis=0, tiled=True,
    ).reshape(total, local_exp)
    x = gather_all(tokens, groups, halves)
    d = gather_all(cotangent, groups, halves)
    weight = jnp.repeat(mine.astype(f32), units, axis=1)

    wg = w_gate.reshape(local_exp * units, width)
    wu = w_up.reshape(local_exp * units, width)
    wd = w_down.reshape(local_exp * units, width)
    nt = (((1,), (1,)), ((), ()))
    tn = (((0,), (0,)), ((), ()))
    gate = lax.dot_general(x, wg, nt, preferred_element_type=f32)
    upval = lax.dot_general(x, wu, nt, preferred_element_type=f32)
    raw = lax.dot_general(d, wd, nt, preferred_element_type=f32)
    sig = jax.nn.sigmoid(gate)
    act = gate * sig
    hidden = act * upval
    score = jnp.sum((hidden * raw).reshape(total, local_exp, units), axis=2)
    dact = weight * raw
    hp = (weight * hidden).astype(jnp.bfloat16)
    dgate = (dact * upval * sig * (1.0 + gate * (1.0 - sig))).astype(jnp.bfloat16)
    dup = (dact * act).astype(jnp.bfloat16)
    part = lax.dot_general(
        jnp.concatenate([dgate, dup], axis=1), jnp.concatenate([wg, wu], axis=0),
        (((1,), (0,)), ((), ())), preferred_element_type=f32,
    ).astype(jnp.bfloat16)
    part = part.reshape(groups, tok_rows, halves, quarter).transpose(0, 2, 1, 3)
    grad_tokens = lax.psum_scatter(
        part.reshape(groups * halves * tok_rows, quarter), BOTH,
        scatter_dimension=0, tiled=True,
    )
    sent = jnp.broadcast_to(
        score.reshape(groups, 1, tok_rows, local_exp), (groups, halves, tok_rows, local_exp)
    ).reshape(groups * halves, tok_rows * local_exp)
    back = lax.all_to_all(sent, BOTH, split_axis=0, concat_axis=0, tiled=True)
    back = jnp.sum(back.reshape(groups, halves, tok_rows, local_exp), axis=1)
    back = back.transpose(1, 0, 2).reshape(tok_rows, 1, experts)
    grad_prob = jnp.sum(jnp.where(hit, back, 0), axis=2)
    shape = (local_exp, units, width)
    grad_gate = lax.dot_general(dgate, x, tn, preferred_element_type=f32).astype(jnp.bfloat16)
    grad_up = lax.dot_general(dup, x, tn, preferred_element_type=f32).astype(jnp.bfloat16)
    grad_down = lax.dot_general(hp, d, tn, preferred_element_type=f32).astype(jnp.bfloat16)
    return (
        grad_tokens,
        grad_prob,
        grad_gate.reshape(shape),
        grad_up.reshape(shape),
        grad_down.reshape(shape),
    )


def solution(mesh):
    in_specs = (
        P("expert", "half"),
        P("expert", "half"),
        P("expert", None),
        P("expert", None),
        P("expert", "half", None),
        P("expert", "half", None),
        P("expert", "half", None),
    )
    out_specs = (
        P("expert", "half"),
        P("expert", None),
        P("expert", "half", None),
        P("expert", "half", None),
        P("expert", "half", None),
    )
    return jax.shard_map(
        per_device, mesh=mesh, in_specs=in_specs, out_specs=out_specs, check_vma=False
    )
```

```python
import functools

import jax
import jax.numpy as jnp
from jax import lax
from jax.experimental import pallas as pl
from jax.experimental.pallas import tpu as pltpu
from jax.sharding import PartitionSpec as P

BOTH = ("expert", "half")


def gather_all(block, groups, halves):
    rows, quarter = block.shape
    parts = lax.all_gather(block, BOTH, axis=0).reshape(groups, halves, rows, quarter)
    return parts.transpose(0, 2, 1, 3).reshape(groups * rows, halves * quarter)


LANES = 128
VMEM_BYTES = 48 << 20
DRAIN_BYTES = 1 << 20
MESH = pl.DeviceIdType.MESH


def place(groups):
    e, h = lax.axis_index("expert"), lax.axis_index("half")
    return lax.div(e, 2), lax.rem(e, 2), lax.div(h, 2), lax.rem(h, 2)


def across(z, step):
    bit = 1
    while bit <= step:
        if step & bit:
            z = z + bit * (1 - 2 * lax.rem(lax.div(z, bit), 2))
        bit *= 2
    return z


def greet(peers):
    barrier = pltpu.get_barrier_semaphore()
    for peer in peers:
        pl.semaphore_signal(barrier, inc=1, device_id=peer, device_id_type=MESH)
    pl.semaphore_wait(barrier, len(peers))


def fused_kernel(
    groups, halves, local_exp, tok_ref, cot_ref, route_ref, prob_ref, wg_ref, wu_ref, wd_ref,
    gt_ref, gp_ref, gg_ref, gu_ref, gd_ref,
    xb, db, wgu, wsides, wdn, gates, raws, dgu, hps, turned, route_in, prob_in, tab_own, tab_in, score, back,
    psend, own, cin, acc, xin0, yin0, yin1, xin1, t0, t1, fin, zin,
    first_send, second_send, core_send, rest_send, pass_send, z_send, z_sem, p_sem, q_sem, c_sem, own_sem, w_sem,
    tab_send, tab_recv, score_send, score_recv,
    part_send, part_recv, hop_send, hop_recv, last_send, last_recv,
):
    line = groups // 2
    z, y, x, c = place(groups)
    e, h = 2 * z + y, 2 * x + c
    rows, quarter = tok_ref.shape
    wide = quarter // 2
    hidden_rows, width = wg_ref.shape
    units = hidden_rows // local_exp
    experts = local_exp * groups
    top = route_ref.shape[0]
    f32, b16 = jnp.float32, tok_ref.dtype
    nt = (((1,), (1,)), ((), ()))
    nn = (((1,), (0,)), ((), ()))
    y_peer = (2 * z + 1 - y, h)
    x_peer = (e, 2 * (1 - x) + c)
    c_peer = (e, 2 * x + 1 - c)

    def local(src, dst, sem):
        copy = pltpu.make_async_copy(src, dst, sem)
        copy.start()
        return copy

    def slot(out, s, yy, xx, cc):
        row = pl.multiple_of((2 * s + yy) * rows, rows)
        col = pl.multiple_of((2 * xx + cc) * quarter, quarter)
        return out.at[pl.ds(row, rows), pl.ds(col, quarter)]

    pair = ((tok_ref, xb), (cot_ref, db))

    def at(a, s, kind, cc):
        over = (kind % 2, kind // 2) if a == 0 else (kind // 2, kind % 2)
        return slot(pair[a][1], s, 1 - y if over[0] else y, 1 - x if over[1] else x, cc)

    mine = [local(pair[a][0], at(a, 0, 0, c), own_sem.at[1 + a]) for a in range(2)]

    small = [local(route_ref, route_in, w_sem.at[3]), local(prob_ref, prob_in, w_sem.at[4])]
    for copy in small:
        copy.wait()
    route_t = route_in[...]
    prob_t = prob_in[...].astype(f32)
    row_of = lax.broadcasted_iota(jnp.int32, (experts, rows), 0)
    table = jnp.zeros((experts, rows), f32)
    for k in range(top):
        table = table + jnp.where(row_of == route_t[k:k + 1, :], prob_t[k:k + 1, :], 0.0)
    tab_own[...] = table
    tab_in[0, 0] = table

    greet([
        (lax.rem(e + i, groups), lax.rem(h + j, halves))
        for i in range(groups) for j in range(halves) if i + j
    ])
    sends, owns = [], []

    def push(src, dst, peer, number, sem):
        copy = pltpu.make_async_remote_copy(
            src_ref=src, dst_ref=dst, send_sem=number, recv_sem=sem,
            device_id=peer, device_id_type=MESH,
        )
        copy.start()
        sends.append(copy)
        return copy

    def arrived(dst, sem):
        pltpu.make_async_remote_copy(
            src_ref=dst, dst_ref=dst, send_sem=own_sem.at[0], recv_sem=sem,
            device_id=c_peer, device_id_type=MESH,
        ).wait_recv()

    hops = ((y_peer, x_peer), (x_peer, y_peer))

    def along(s):
        return (2 * across(z, s) + y, h)

    middle_chip = lax.div(z + 1, 2) == 1
    passed = []

    def pass_on(src, s_to, step, a, number):
        copy = pltpu.make_async_remote_copy(
            src_ref=src, dst_ref=at(a, s_to, 0, c), send_sem=pass_send.at[a, number],
            recv_sem=z_sem.at[a, s_to], device_id=along(step), device_id_type=MESH,
        )
        passed.append(copy)
        return copy

    def start_middle():
        copies = [pass_on(at(a, 0, 0, c), 3, 3, a, 0) for a in range(2)]

        @pl.when(middle_chip)
        def _():
            for copy in copies:
                copy.start()

    def relay_near():
        inner = [pass_on(at(a, 1, 0, c), 2, 3, a, 1) for a in range(2)]
        outer = [pass_on(at(a, 3, 0, c), 2, 1, a, 2) for a in range(2)]

        @pl.when(middle_chip)
        def _():
            for a in range(2):
                arrived(at(a, 1, 0, c), z_sem.at[a, 1])
                inner[a].start()
                arrived(at(a, 3, 0, c), z_sem.at[a, 3])
                outer[a].start()

    def gather_own(s):
        have = [at(a, s, 0, c) for a in range(2)]
        far = [pass_on(at(a, 2, 0, c), 3, 1, a, 3) for a in range(2)] if s == 2 else None
        for a in range(2):
            if s == 2:
                arrived(have[a], z_sem.at[a, s])

                @pl.when(middle_chip)
                def _():
                    far[a].start()
            elif s > 0:
                @pl.when(jnp.logical_not(middle_chip))
                def _():
                    arrived(have[a], z_sem.at[a, s])
            if s != 1:
                push(have[a], have[a], hops[a][0], first_send.at[a, s], p_sem.at[a, s])
            if s > 0:
                push(have[a], have[a], hops[a][1], second_send.at[a, s], q_sem.at[a, s])
        for a in range(2):
            if s == 0:
                push(have[a], have[a], hops[a][1], second_send.at[a, s], q_sem.at[a, s])
        for a in range(2):
            push(have[a], have[a], c_peer, core_send.at[a, s], c_sem.at[a, s])

    def gather_first(s):
        there = [at(a, s, 1, c) for a in range(2)]
        for a in range(2):
            arrived(there[a], p_sem.at[a, s])
            if s != 1:
                push(
                    there[a], there[a], hops[a][1],
                    second_send.at[a, line + s], q_sem.at[a, line + s],
                )
        for a in range(2):
            push(there[a], there[a], c_peer, core_send.at[a, line + s], c_sem.at[a, line + s])

    def gather_second(s, kind):
        for a in range(2):
            there = at(a, s, kind, c)
            arrived(there, q_sem.at[a, (kind - 2) * line + s])
            push(there, there, c_peer, core_send.at[a, kind * line + s], c_sem.at[a, kind * line + s])

    def send_plane(s):
        for a in range(2):
            push(at(a, 0, 0, c), at(a, s, 0, c), along(s), z_send.at[a, s], z_sem.at[a, s])

    def send_rest(kind):
        for a in range(2):
            sem = p_sem.at[a, 1] if kind == 1 else q_sem.at[a, line + 1]
            push(at(a, 0, kind, c), at(a, 1, kind, c), along(1), rest_send.at[a, kind // 2], sem)

    def gather_core(s):
        for a in range(2):
            for kind in range(4):
                arrived(at(a, s, kind, 1 - c), c_sem.at[a, kind * line + s])

    def plane(s):
        return pl.ds(2 * s * rows, 2 * rows)

    def forward(s):
        for r in range(2):
            part = pl.ds(r * hidden_rows, hidden_rows)
            gates[part, :] = lax.dot_general(
                wgu[part, :], xb[plane(s), :], nt, preferred_element_type=f32
            )

    def middle(s):
        for r in range(2):
            part = pl.ds(r * hidden_rows // 2, hidden_rows // 2)
            raws[part, :] = lax.dot_general(
                wdn[part, :], db[plane(s), :], nt, preferred_element_type=f32
            )
        chunk = 32 if units % 32 == 0 else 16
        expert_of = lax.broadcasted_iota(jnp.int32, (experts, rows), 0)
        lane = pl.ds(2 * s * rows, 2 * rows)
        sums = []
        tabs = [tab_in[s, y], tab_in[s, 1 - y]]
        for l in range(local_exp):
            weight = jnp.concatenate([
                jnp.sum(jnp.where(expert_of == local_exp * e + l, t, 0.0), axis=0, keepdims=True)
                for t in tabs
            ], axis=1)

            def step(i, total, l=l, weight=weight):
                at_row = pl.multiple_of(l * units + i * chunk, chunk)
                up_row = pl.multiple_of(hidden_rows + l * units + i * chunk, chunk)
                g = gates[pl.ds(at_row, chunk), :]
                u = gates[pl.ds(up_row, chunk), :]
                r = raws[pl.ds(at_row, chunk), :]
                sig = jax.nn.sigmoid(g)
                act = g * sig
                hidden = act * u
                dact = weight * r
                hps[pl.ds(at_row, chunk), lane] = (weight * hidden).astype(b16)
                dgu[pl.ds(at_row, chunk), lane] = (
                    dact * u * sig * (1.0 + g * (1.0 - sig))
                ).astype(b16)
                dgu[pl.ds(up_row, chunk), lane] = (dact * act).astype(b16)
                return total + jnp.sum((hidden * r).reshape(chunk // 8, 8, 2 * rows), axis=0)

            total = lax.fori_loop(0, units // chunk, step, jnp.zeros((8, 2 * rows), f32))
            sums.append(jnp.sum(total, axis=0, keepdims=True))
        sub = lax.broadcasted_iota(jnp.int32, (8, rows), 0)
        for yy in range(2):
            block = jnp.zeros((8, rows), f32)
            for l in range(local_exp):
                block = jnp.where(sub == l, sums[l][:, yy * rows:(yy + 1) * rows], block)
            score[s, yy] = block
        turned[...] = dgu[:, lane].T

    def part_of(side):
        cols = pl.ds(side * 2 * quarter, 2 * quarter)
        return lax.dot_general(
            turned[...], wsides[:, cols], nn, preferred_element_type=f32
        ).astype(b16)

    def send_part(s):
        theirs = part_of(0)
        for xx in range(2):
            psend[s, xx] = theirs[:, xx * quarter:(xx + 1) * quarter]
            push(psend.at[s, xx], cin.at[s, xx], c_peer, part_send.at[s, xx], part_recv.at[s, xx])
        mine = part_of(1)
        for xx in range(2):
            own[s, xx] = mine[:, xx * quarter:(xx + 1) * quarter]

    def flipped(dy):
        return 1 - y if dy else y

    def send_score(s):
        for dy in range(2):
            for j in range(halves):
                if s + dy + j == 0:
                    owns.append(local(score.at[0, y], back.at[0, 0, h], own_sem.at[3]))
                    continue
                push(
                    score.at[s, flipped(dy)], back.at[s, dy, h],
                    (2 * across(z, s) + flipped(dy), lax.rem(h + j, halves)),
                    score_send.at[s, dy, j], score_recv.at[s, dy, j],
                )

    step_rows = 32

    def row_loop(count):
        return pl.loop(0, count // step_rows)

    def some(i):
        return pl.ds(pl.multiple_of(i * step_rows, step_rows), step_rows)

    def settle_core(s):
        for xx in range(2):
            arrived(cin.at[s, xx], part_recv.at[s, xx])

            @row_loop(2 * rows)
            def _(i):
                both = own[s, xx, some(i)].astype(f32) + cin[s, xx, some(i)].astype(f32)
                acc[s, 0, xx, some(i)] = both[:, :wide].astype(b16)
                acc[s, 1, xx, some(i)] = both[:, wide:].astype(b16)

        push(acc.at[s, 0, 1 - x], xin0.at[s], x_peer, hop_send.at[s, 0], hop_recv.at[s, 0])
        away = pl.ds(pl.multiple_of((1 - y) * rows, rows), rows)
        push(acc.at[s, 1, :, away], yin1.at[s], y_peer, hop_send.at[s, 1], hop_recv.at[s, 1])

    def settle_first(s):
        arrived(xin0.at[s], hop_recv.at[s, 0])

        @row_loop(2 * rows)
        def _(i):
            t0[s, some(i)] = (
                acc[s, 0, x, some(i)].astype(f32) + xin0[s, some(i)].astype(f32)
            ).astype(b16)

        away = pl.ds(pl.multiple_of((1 - y) * rows, rows), rows)
        push(t0.at[s, away], yin0.at[s], y_peer, hop_send.at[s, 2], hop_recv.at[s, 2])
        arrived(yin1.at[s], hop_recv.at[s, 1])

        @row_loop(rows)
        def _(i):
            here = pl.ds(pl.multiple_of(y * rows + i * step_rows, step_rows), step_rows)
            for xx in range(2):
                t1[s, xx, some(i)] = (
                    acc[s, 1, xx, here].astype(f32) + yin1[s, xx, some(i)].astype(f32)
                ).astype(b16)

        push(t1.at[s, 1 - x], xin1.at[s], x_peer, hop_send.at[s, 3], hop_recv.at[s, 3])

    def settle_second(s):
        arrived(yin0.at[s], hop_recv.at[s, 2])
        arrived(xin1.at[s], hop_recv.at[s, 3])

        @row_loop(rows)
        def _(i):
            here = pl.ds(pl.multiple_of(y * rows + i * step_rows, step_rows), step_rows)
            fin[s, some(i), :wide] = (
                t0[s, here].astype(f32) + yin0[s, some(i)].astype(f32)
            ).astype(b16)
            fin[s, some(i), wide:] = (
                t1[s, x, some(i)].astype(f32) + xin1[s, some(i)].astype(f32)
            ).astype(b16)

        if s > 0:
            push(fin.at[s], zin.at[s], (2 * across(z, s) + y, h), last_send.at[s], last_recv.at[s])

    cut = quarter

    def grads_in(n):
        cols = pl.ds(n * cut, cut)
        both = lax.dot_general(dgu[...], xb[:, cols], nn, preferred_element_type=f32).astype(b16)
        gg_ref[:, cols] = both[:hidden_rows]
        gu_ref[:, cols] = both[hidden_rows:]

    def grads_out(n):
        cols = pl.ds(n * cut, cut)
        gd_ref[:, cols] = lax.dot_general(
            hps[...], db[:, cols], nn, preferred_element_type=f32
        ).astype(b16)

    for copy in mine:
        copy.wait()
    def send_table():
        for s in range(line):
            for dy in range(2):
                if s + dy:
                    push(
                        tab_own, tab_in.at[s, dy], (2 * across(z, s) + flipped(dy), h),
                        tab_send.at[s, dy], tab_recv.at[s, dy],
                    )

    def table_in(s):
        for dy in range(2):
            if s + dy:
                arrived(tab_in.at[s, dy], tab_recv.at[s, dy])

    def finish(s):
        middle(s)
        send_part(s)
        send_score(s)

    gather_own(0)
    send_plane(1)
    start_middle()
    send_table()
    weights = [
        local(wg_ref, wgu.at[pl.ds(0, hidden_rows)], w_sem.at[0]),
        local(wu_ref, wgu.at[pl.ds(hidden_rows, hidden_rows)], w_sem.at[1]),
        local(wd_ref, wdn, w_sem.at[2]),
    ]
    for r, ref in enumerate((wg_ref, wu_ref)):
        for n in range(4):
            q = 2 * (n % 2) + (c if n // 2 else 1 - c)
            weights.append(local(
                ref.at[:, pl.ds(pl.multiple_of(q * quarter, quarter), quarter)],
                wsides.at[pl.ds(r * hidden_rows, hidden_rows), pl.ds(n * quarter, quarter)],
                w_sem.at[5 + 4 * r + n],
            ))
    gather_first(0)
    relay_near()
    gather_own(1)
    gather_second(0, 2)
    gather_second(0, 3)
    gather_core(0)
    gather_own(2)
    send_rest(1)
    send_rest(3)
    for copy in weights:
        copy.wait()
    table_in(0)
    forward(0)
    gather_second(1, 2)
    finish(0)
    gather_first(2)
    gather_own(3)
    settle_core(0)
    gather_second(2, 2)
    gather_second(2, 3)
    gather_core(2)
    table_in(2)
    forward(2)
    gather_first(3)
    finish(2)
    settle_first(0)
    gather_first(1)
    settle_core(2)
    gather_second(3, 2)
    gather_second(3, 3)
    gather_second(1, 3)
    gather_core(3)
    table_in(3)
    forward(3)
    settle_second(0)
    middle(3)
    send_part(3)
    settle_first(2)
    gather_core(1)
    table_in(1)
    forward(1)
    settle_core(3)
    middle(1)
    send_part(1)
    settle_second(2)
    settle_first(3)
    settle_core(1)
    send_score(3)
    send_score(1)
    grads_in(0)
    grads_in(1)
    settle_second(3)
    grads_in(2)
    grads_in(3)
    settle_first(1)
    grads_out(0)
    grads_out(1)
    settle_second(1)
    grads_out(2)
    grads_out(3)

    for copy in owns:
        copy.wait()
    for s in range(line):
        for dy in range(2):
            for j in range(halves):
                if s + dy + j:
                    arrived(
                        back.at[s, dy, lax.rem(h + halves - j, halves)], score_recv.at[s, dy, j]
                    )
    total = jnp.zeros((top, rows), f32)
    for s in range(line):
        for dy in range(2):
            block = back[s, dy, 0]
            for j in range(1, halves):
                block = block + back[s, dy, j]
            first = local_exp * (2 * across(z, s) + flipped(dy))
            for l in range(local_exp):
                total = total + jnp.where(
                    route_t == first + l, block[l:l + 1, :], 0.0
                )
    gp_ref[...] = total
    for s in range(1, line):
        arrived(zin.at[s], last_recv.at[s])

    @row_loop(rows)
    def _(i):
        whole = fin[0, some(i)].astype(f32)
        for s in range(1, line):
            whole = whole + zin[s, some(i)].astype(f32)
        gt_ref[some(i)] = whole.astype(b16)

    for copy in sends:
        copy.wait_send()

    @pl.when(middle_chip)
    def _():
        for copy in passed:
            copy.wait_send()


def fused(tokens, cotangent, route, prob, wg, wu, wd, groups, halves, local_exp):
    rows, quarter = tokens.shape
    line, wide = groups // 2, quarter // 2
    hidden_rows, width = wg.shape
    experts, top = local_exp * groups, route.shape[0]
    b16, f32 = tokens.dtype, jnp.float32
    dma = pltpu.SemaphoreType.DMA
    vmem = pl.BlockSpec(memory_space=pltpu.VMEM)
    hbm = pl.BlockSpec(memory_space=pltpu.HBM)
    total = groups * rows
    grad = jax.ShapeDtypeStruct((hidden_rows, width), b16)
    return pl.pallas_call(
        functools.partial(fused_kernel, groups, halves, local_exp),
        out_shape=(
            jax.ShapeDtypeStruct((rows, quarter), b16),
            jax.ShapeDtypeStruct((top, rows), f32),
            grad, grad, grad,
        ),
        in_specs=[hbm] * 7,
        out_specs=[vmem] * 5,
        scratch_shapes=[
            pltpu.VMEM((total, width), b16),
            pltpu.VMEM((total, width), b16),
            pltpu.VMEM((2 * hidden_rows, width), b16),
            pltpu.VMEM((2 * hidden_rows, width), b16),
            pltpu.VMEM((hidden_rows, width), b16),
            pltpu.VMEM((2 * hidden_rows, 2 * rows), f32),
            pltpu.VMEM((hidden_rows, 2 * rows), f32),
            pltpu.VMEM((2 * hidden_rows, total), b16),
            pltpu.VMEM((hidden_rows, total), b16),
            pltpu.VMEM((2 * rows, 2 * hidden_rows), b16),
            pltpu.VMEM(route.shape, route.dtype),
            pltpu.VMEM(prob.shape, prob.dtype),
            pltpu.VMEM((experts, rows), f32),
            pltpu.VMEM((line, 2, experts, rows), f32),
            pltpu.VMEM((line, 2, 8, rows), f32),
            pltpu.VMEM((line, 2, halves, 8, rows), f32),
            pltpu.VMEM((line, 2, 2 * rows, quarter), b16),
            pltpu.VMEM((line, 2, 2 * rows, quarter), b16),
            pltpu.VMEM((line, 2, 2 * rows, quarter), b16),
            pltpu.VMEM((line, 2, 2, 2 * rows, wide), b16),
            pltpu.VMEM((line, 2 * rows, wide), b16),
            pltpu.VMEM((line, rows, wide), b16),
            pltpu.VMEM((line, 2, rows, wide), b16),
            pltpu.VMEM((line, rows, wide), b16),
            pltpu.VMEM((line, 2 * rows, wide), b16),
            pltpu.VMEM((line, 2, rows, wide), b16),
            pltpu.VMEM((line, rows, quarter), b16),
            pltpu.VMEM((line, rows, quarter), b16),
            dma((2, line)), dma((2, 2 * line)), dma((2, 4 * line)), dma((2, 2)), dma((2, 4)), dma((2, line)),
            dma((2, line)), dma((2, line)), dma((2, 2 * line)), dma((2, 4 * line)),
            dma((4,)), dma((13,)),
            dma((line, 2)), dma((line, 2)),
            dma((line, 2, halves)), dma((line, 2, halves)),
            dma((line, 2)), dma((line, 2)),
            dma((line, 4)), dma((line, 4)),
            dma((line,)), dma((line,)),
        ],
        compiler_params=pltpu.CompilerParams(
            collective_id=0, has_side_effects=True, vmem_limit_bytes=VMEM_BYTES
        ),
    )(tokens, cotangent, route, prob, wg, wu, wd)


def drain_kernel(count, *refs):
    sources, targets, sem = refs[:count], refs[count:2 * count], refs[2 * count]
    copies = [pltpu.make_async_copy(a, b, sem.at[i]) for i, (a, b) in enumerate(zip(sources, targets))]
    for copy in copies:
        copy.start()
    for copy in copies:
        copy.wait()


def drain(arrays):
    count = len(arrays)
    return pl.pallas_call(
        functools.partial(drain_kernel, count),
        out_shape=[jax.ShapeDtypeStruct(a.shape, a.dtype) for a in arrays],
        in_specs=[pl.BlockSpec(memory_space=pltpu.VMEM)] * count,
        out_specs=[pl.BlockSpec(memory_space=pl.ANY)] * count,
        scratch_shapes=[pltpu.SemaphoreType.DMA((count,))],
        compiler_params=pltpu.CompilerParams(vmem_limit_bytes=DRAIN_BYTES),
    )(*arrays)


def per_device(tokens, cotangent, route, prob, w_gate, w_up, w_down):
    tok_rows, quarter = tokens.shape
    local_exp, units, width = w_gate.shape
    groups = lax.axis_size("expert")
    halves = lax.axis_size("half")
    experts = local_exp * groups
    total = groups * tok_rows
    f32 = jnp.float32
    me = lax.axis_index("expert")

    fast = (
        groups == 2 * halves and halves == 2 * 2 and width == 4 * quarter
        and tok_rows == LANES and quarter % (2 * LANES) == 0
        and units % 32 == 0 and local_exp <= 8 and experts <= 2 * LANES and route.shape[1] <= 8
        and 2 * total * width * 2 + 12 * local_exp * units * width <= VMEM_BYTES // 2
    )
    if fast:
        flat = (local_exp * units, width)
        results = fused(
            *[pltpu.with_memory_space_constraint(v, pltpu.HBM) for v in (tokens, cotangent, route.T, prob.T)], w_gate.reshape(flat), w_up.reshape(flat),
            w_down.reshape(flat), groups, halves, local_exp,
        )
        grad_tokens, grad_prob, *grads = drain(results)
        grads = [g.reshape(local_exp, units, width) for g in grads]
        return (grad_tokens, grad_prob.T, *grads)

    hit = route[:, :, None] == jnp.arange(experts, dtype=route.dtype)
    table = jnp.sum(jnp.where(hit, prob[:, :, None], 0).astype(f32), axis=1).astype(prob.dtype)
    mine = lax.all_to_all(
        table.reshape(tok_rows, groups, local_exp), "expert",
        split_axis=1, concat_axis=0, tiled=True,
    ).reshape(total, local_exp)
    x = gather_all(tokens, groups, halves)
    d = gather_all(cotangent, groups, halves)
    weight = jnp.repeat(mine.astype(f32), units, axis=1)

    wg = w_gate.reshape(local_exp * units, width)
    wu = w_up.reshape(local_exp * units, width)
    wd = w_down.reshape(local_exp * units, width)
    nt = (((1,), (1,)), ((), ()))
    tn = (((0,), (0,)), ((), ()))
    gate = lax.dot_general(x, wg, nt, preferred_element_type=f32)
    upval = lax.dot_general(x, wu, nt, preferred_element_type=f32)
    raw = lax.dot_general(d, wd, nt, preferred_element_type=f32)
    sig = jax.nn.sigmoid(gate)
    act = gate * sig
    hidden = act * upval
    score = jnp.sum((hidden * raw).reshape(total, local_exp, units), axis=2)
    dact = weight * raw
    hp = (weight * hidden).astype(jnp.bfloat16)
    dgate = (dact * upval * sig * (1.0 + gate * (1.0 - sig))).astype(jnp.bfloat16)
    dup = (dact * act).astype(jnp.bfloat16)
    part = lax.dot_general(
        jnp.concatenate([dgate, dup], axis=1), jnp.concatenate([wg, wu], axis=0),
        (((1,), (0,)), ((), ())), preferred_element_type=f32,
    ).astype(jnp.bfloat16)
    part = part.reshape(groups, tok_rows, halves, quarter).transpose(0, 2, 1, 3)
    grad_tokens = lax.psum_scatter(
        part.reshape(groups * halves * tok_rows, quarter), BOTH,
        scatter_dimension=0, tiled=True,
    )
    sent = jnp.broadcast_to(
        score.reshape(groups, 1, tok_rows, local_exp), (groups, halves, tok_rows, local_exp)
    ).reshape(groups * halves, tok_rows * local_exp)
    back = lax.all_to_all(sent, BOTH, split_axis=0, concat_axis=0, tiled=True)
    back = jnp.sum(back.reshape(groups, halves, tok_rows, local_exp), axis=1)
    back = back.transpose(1, 0, 2).reshape(tok_rows, 1, experts)
    grad_prob = jnp.sum(jnp.where(hit, back, 0), axis=2)
    shape = (local_exp, units, width)
    grad_gate = lax.dot_general(dgate, x, tn, preferred_element_type=f32).astype(jnp.bfloat16)
    grad_up = lax.dot_general(dup, x, tn, preferred_element_type=f32).astype(jnp.bfloat16)
    grad_down = lax.dot_general(hp, d, tn, preferred_element_type=f32).astype(jnp.bfloat16)
    return (
        grad_tokens,
        grad_prob,
        grad_gate.reshape(shape),
        grad_up.reshape(shape),
        grad_down.reshape(shape),
    )


def solution(mesh):
    in_specs = (
        P("expert", "half"),
        P("expert", "half"),
        P("expert", None),
        P("expert", None),
        P("expert", "half", None),
        P("expert", "half", None),
        P("expert", "half", None),
    )
    out_specs = (
        P("expert", "half"),
        P("expert", None),
        P("expert", "half", None),
        P("expert", "half", None),
        P("expert", "half", None),
    )
    return jax.shard_map(
        per_device, mesh=mesh, in_specs=in_specs, out_specs=out_specs, check_vma=False
    )
```

```python
import functools

import jax
import jax.numpy as jnp
from jax import lax
from jax.experimental import pallas as pl
from jax.experimental.pallas import tpu as pltpu
from jax.sharding import PartitionSpec as P

BOTH = ("expert", "half")


def gather_all(block, groups, halves):
    rows, quarter = block.shape
    parts = lax.all_gather(block, BOTH, axis=0).reshape(groups, halves, rows, quarter)
    return parts.transpose(0, 2, 1, 3).reshape(groups * rows, halves * quarter)


LANES = 128
VMEM_BYTES = 48 << 20
DRAIN_BYTES = 1 << 20
MESH = pl.DeviceIdType.MESH


def place(groups):
    e, h = lax.axis_index("expert"), lax.axis_index("half")
    return lax.div(e, 2), lax.rem(e, 2), lax.div(h, 2), lax.rem(h, 2)


def across(z, step):
    bit = 1
    while bit <= step:
        if step & bit:
            z = z + bit * (1 - 2 * lax.rem(lax.div(z, bit), 2))
        bit *= 2
    return z


def greet(peers):
    barrier = pltpu.get_barrier_semaphore()
    for peer in peers:
        pl.semaphore_signal(barrier, inc=1, device_id=peer, device_id_type=MESH)
    pl.semaphore_wait(barrier, len(peers))


def fused_kernel(
    groups, halves, local_exp, tok_ref, cot_ref, route_ref, prob_ref, wg_ref, wu_ref, wd_ref,
    gt_ref, gp_ref, gg_ref, gu_ref, gd_ref,
    xb, db, wgu, wsides, wdn, gates, raws, dgu, hps, turned, route_in, prob_in, tab_own, tab_in, score, back,
    psend, own, cin, acc, xin0, yin0, yin1, xin1, t0, t1, fin, zin,
    first_send, second_send, core_send, rest_send, pass_send, z_send, z_sem, p_sem, q_sem, c_sem, own_sem, w_sem,
    tab_send, tab_recv, score_send, score_recv,
    part_send, part_recv, hop_send, hop_recv, last_send, last_recv,
):
    line = groups // 2
    z, y, x, c = place(groups)
    e, h = 2 * z + y, 2 * x + c
    rows, quarter = tok_ref.shape
    wide = quarter // 2
    hidden_rows, width = wg_ref.shape
    units = hidden_rows // local_exp
    experts = local_exp * groups
    top = route_ref.shape[0]
    f32, b16 = jnp.float32, tok_ref.dtype
    nt = (((1,), (1,)), ((), ()))
    nn = (((1,), (0,)), ((), ()))
    y_peer = (2 * z + 1 - y, h)
    x_peer = (e, 2 * (1 - x) + c)
    c_peer = (e, 2 * x + 1 - c)

    def local(src, dst, sem):
        copy = pltpu.make_async_copy(src, dst, sem)
        copy.start()
        return copy

    def slot(out, s, yy, xx, cc):
        row = pl.multiple_of((2 * s + yy) * rows, rows)
        col = pl.multiple_of((2 * xx + cc) * quarter, quarter)
        return out.at[pl.ds(row, rows), pl.ds(col, quarter)]

    pair = ((tok_ref, xb), (cot_ref, db))

    def at(a, s, kind, cc):
        over = (kind % 2, kind // 2) if a == 0 else (kind // 2, kind % 2)
        return slot(pair[a][1], s, 1 - y if over[0] else y, 1 - x if over[1] else x, cc)

    mine = [local(pair[a][0], at(a, 0, 0, c), own_sem.at[1 + a]) for a in range(2)]

    small = [local(route_ref, route_in, w_sem.at[3]), local(prob_ref, prob_in, w_sem.at[4])]
    for copy in small:
        copy.wait()
    route_t = route_in[...]
    prob_t = prob_in[...].astype(f32)
    row_of = lax.broadcasted_iota(jnp.int32, (experts, rows), 0)
    table = jnp.zeros((experts, rows), f32)
    for k in range(top):
        table = table + jnp.where(row_of == route_t[k:k + 1, :], prob_t[k:k + 1, :], 0.0)
    tab_own[...] = table
    tab_in[0, 0] = table

    greet([
        (lax.rem(e + i, groups), lax.rem(h + j, halves))
        for i in range(groups) for j in range(halves) if i + j
    ])
    sends, owns = [], []

    def push(src, dst, peer, number, sem):
        copy = pltpu.make_async_remote_copy(
            src_ref=src, dst_ref=dst, send_sem=number, recv_sem=sem,
            device_id=peer, device_id_type=MESH,
        )
        copy.start()
        sends.append(copy)
        return copy

    def arrived(dst, sem):
        pltpu.make_async_remote_copy(
            src_ref=dst, dst_ref=dst, send_sem=own_sem.at[0], recv_sem=sem,
            device_id=c_peer, device_id_type=MESH,
        ).wait_recv()

    hops = ((y_peer, x_peer), (x_peer, y_peer))

    def along(s):
        return (2 * across(z, s) + y, h)

    middle_chip = lax.div(z + 1, 2) == 1
    passed = []

    def pass_on(src, s_to, step, a, number):
        copy = pltpu.make_async_remote_copy(
            src_ref=src, dst_ref=at(a, s_to, 0, c), send_sem=pass_send.at[a, number],
            recv_sem=z_sem.at[a, s_to], device_id=along(step), device_id_type=MESH,
        )
        passed.append(copy)
        return copy

    def start_middle():
        copies = [pass_on(at(a, 0, 0, c), 3, 3, a, 0) for a in range(2)]

        @pl.when(middle_chip)
        def _():
            for copy in copies:
                copy.start()

    def relay_near():
        inner = [pass_on(at(a, 1, 0, c), 2, 3, a, 1) for a in range(2)]
        outer = [pass_on(at(a, 3, 0, c), 2, 1, a, 2) for a in range(2)]

        @pl.when(middle_chip)
        def _():
            for a in range(2):
                arrived(at(a, 1, 0, c), z_sem.at[a, 1])
                inner[a].start()
                arrived(at(a, 3, 0, c), z_sem.at[a, 3])
                outer[a].start()

    def gather_own(s):
        have = [at(a, s, 0, c) for a in range(2)]
        far = [pass_on(at(a, 2, 0, c), 3, 1, a, 3) for a in range(2)] if s == 2 else None
        for a in range(2):
            if s == 2:
                arrived(have[a], z_sem.at[a, s])

                @pl.when(middle_chip)
                def _():
                    far[a].start()
            elif s > 0:
                @pl.when(jnp.logical_not(middle_chip))
                def _():
                    arrived(have[a], z_sem.at[a, s])
            if s != 1:
                push(have[a], have[a], hops[a][0], first_send.at[a, s], p_sem.at[a, s])
            if s > 0:
                push(have[a], have[a], hops[a][1], second_send.at[a, s], q_sem.at[a, s])
        for a in range(2):
            if s == 0:
                push(have[a], have[a], hops[a][1], second_send.at[a, s], q_sem.at[a, s])
        for a in range(2):
            push(have[a], have[a], c_peer, core_send.at[a, s], c_sem.at[a, s])

    def gather_first(s):
        there = [at(a, s, 1, c) for a in range(2)]
        for a in range(2):
            arrived(there[a], p_sem.at[a, s])
            if s != 1:
                push(
                    there[a], there[a], hops[a][1],
                    second_send.at[a, line + s], q_sem.at[a, line + s],
                )
        for a in range(2):
            push(there[a], there[a], c_peer, core_send.at[a, line + s], c_sem.at[a, line + s])

    def gather_second(s, kind):
        for a in range(2):
            there = at(a, s, kind, c)
            arrived(there, q_sem.at[a, (kind - 2) * line + s])
            push(there, there, c_peer, core_send.at[a, kind * line + s], c_sem.at[a, kind * line + s])

    def send_plane(s):
        for a in range(2):
            push(at(a, 0, 0, c), at(a, s, 0, c), along(s), z_send.at[a, s], z_sem.at[a, s])

    def send_rest(kind):
        for a in range(2):
            sem = p_sem.at[a, 1] if kind == 1 else q_sem.at[a, line + 1]
            push(at(a, 0, kind, c), at(a, 1, kind, c), along(1), rest_send.at[a, kind // 2], sem)

    def gather_core(s):
        for a in range(2):
            for kind in range(4):
                arrived(at(a, s, kind, 1 - c), c_sem.at[a, kind * line + s])

    def plane(s):
        return pl.ds(2 * s * rows, 2 * rows)

    def forward(s):
        for r in range(2):
            part = pl.ds(r * hidden_rows, hidden_rows)
            gates[part, :] = lax.dot_general(
                wgu[part, :], xb[plane(s), :], nt, preferred_element_type=f32
            )

    def middle(s):
        for r in range(2):
            part = pl.ds(r * hidden_rows // 2, hidden_rows // 2)
            raws[part, :] = lax.dot_general(
                wdn[part, :], db[plane(s), :], nt, preferred_element_type=f32
            )
        chunk = 32 if units % 32 == 0 else 16
        expert_of = lax.broadcasted_iota(jnp.int32, (experts, rows), 0)
        lane = pl.ds(2 * s * rows, 2 * rows)
        sums = []
        tabs = [tab_in[s, y], tab_in[s, 1 - y]]
        for l in range(local_exp):
            weight = jnp.concatenate([
                jnp.sum(jnp.where(expert_of == local_exp * e + l, t, 0.0), axis=0, keepdims=True)
                for t in tabs
            ], axis=1)

            def step(i, total, l=l, weight=weight):
                at_row = pl.multiple_of(l * units + i * chunk, chunk)
                up_row = pl.multiple_of(hidden_rows + l * units + i * chunk, chunk)
                g = gates[pl.ds(at_row, chunk), :]
                u = gates[pl.ds(up_row, chunk), :]
                r = raws[pl.ds(at_row, chunk), :]
                sig = jax.nn.sigmoid(g)
                act = g * sig
                hidden = act * u
                dact = weight * r
                hps[pl.ds(at_row, chunk), lane] = (weight * hidden).astype(b16)
                dgu[pl.ds(at_row, chunk), lane] = (
                    dact * u * sig * (1.0 + g * (1.0 - sig))
                ).astype(b16)
                dgu[pl.ds(up_row, chunk), lane] = (dact * act).astype(b16)
                return total + jnp.sum((hidden * r).reshape(chunk // 8, 8, 2 * rows), axis=0)

            total = lax.fori_loop(0, units // chunk, step, jnp.zeros((8, 2 * rows), f32))
            sums.append(jnp.sum(total, axis=0, keepdims=True))
        sub = lax.broadcasted_iota(jnp.int32, (8, rows), 0)
        for yy in range(2):
            block = jnp.zeros((8, rows), f32)
            for l in range(local_exp):
                block = jnp.where(sub == l, sums[l][:, yy * rows:(yy + 1) * rows], block)
            score[s, yy] = block
        turned[...] = dgu[:, lane].T

    def part_of(side):
        cols = pl.ds(side * 2 * quarter, 2 * quarter)
        return lax.dot_general(
            turned[...], wsides[:, cols], nn, preferred_element_type=f32
        ).astype(b16)

    def send_part(s):
        theirs = part_of(0)
        for xx in range(2):
            psend[s, xx] = theirs[:, xx * quarter:(xx + 1) * quarter]
            push(psend.at[s, xx], cin.at[s, xx], c_peer, part_send.at[s, xx], part_recv.at[s, xx])
        mine = part_of(1)
        for xx in range(2):
            own[s, xx] = mine[:, xx * quarter:(xx + 1) * quarter]

    def flipped(dy):
        return 1 - y if dy else y

    def send_score(s):
        for dy in range(2):
            for j in range(halves):
                if s + dy + j == 0:
                    owns.append(local(score.at[0, y], back.at[0, 0, h], own_sem.at[3]))
                    continue
                push(
                    score.at[s, flipped(dy)], back.at[s, dy, h],
                    (2 * across(z, s) + flipped(dy), lax.rem(h + j, halves)),
                    score_send.at[s, dy, j], score_recv.at[s, dy, j],
                )

    step_rows = 32

    def row_loop(count):
        return pl.loop(0, count // step_rows)

    def some(i):
        return pl.ds(pl.multiple_of(i * step_rows, step_rows), step_rows)

    def settle_core(s):
        for xx in range(2):
            arrived(cin.at[s, xx], part_recv.at[s, xx])

            @row_loop(2 * rows)
            def _(i):
                both = own[s, xx, some(i)].astype(f32) + cin[s, xx, some(i)].astype(f32)
                acc[s, 0, xx, some(i)] = both[:, :wide].astype(b16)
                acc[s, 1, xx, some(i)] = both[:, wide:].astype(b16)

        push(acc.at[s, 0, 1 - x], xin0.at[s], x_peer, hop_send.at[s, 0], hop_recv.at[s, 0])
        away = pl.ds(pl.multiple_of((1 - y) * rows, rows), rows)
        push(acc.at[s, 1, :, away], yin1.at[s], y_peer, hop_send.at[s, 1], hop_recv.at[s, 1])

    def settle_first(s):
        arrived(xin0.at[s], hop_recv.at[s, 0])

        @row_loop(2 * rows)
        def _(i):
            t0[s, some(i)] = (
                acc[s, 0, x, some(i)].astype(f32) + xin0[s, some(i)].astype(f32)
            ).astype(b16)

        away = pl.ds(pl.multiple_of((1 - y) * rows, rows), rows)
        push(t0.at[s, away], yin0.at[s], y_peer, hop_send.at[s, 2], hop_recv.at[s, 2])
        arrived(yin1.at[s], hop_recv.at[s, 1])

        @row_loop(rows)
        def _(i):
            here = pl.ds(pl.multiple_of(y * rows + i * step_rows, step_rows), step_rows)
            for xx in range(2):
                t1[s, xx, some(i)] = (
                    acc[s, 1, xx, here].astype(f32) + yin1[s, xx, some(i)].astype(f32)
                ).astype(b16)

        push(t1.at[s, 1 - x], xin1.at[s], x_peer, hop_send.at[s, 3], hop_recv.at[s, 3])

    def settle_second(s):
        arrived(yin0.at[s], hop_recv.at[s, 2])
        arrived(xin1.at[s], hop_recv.at[s, 3])

        @row_loop(rows)
        def _(i):
            here = pl.ds(pl.multiple_of(y * rows + i * step_rows, step_rows), step_rows)
            fin[s, some(i), :wide] = (
                t0[s, here].astype(f32) + yin0[s, some(i)].astype(f32)
            ).astype(b16)
            fin[s, some(i), wide:] = (
                t1[s, x, some(i)].astype(f32) + xin1[s, some(i)].astype(f32)
            ).astype(b16)

        if s > 0:
            push(fin.at[s], zin.at[s], (2 * across(z, s) + y, h), last_send.at[s], last_recv.at[s])

    cut = quarter

    def grads_in(n):
        cols = pl.ds(n * cut, cut)
        both = lax.dot_general(dgu[...], xb[:, cols], nn, preferred_element_type=f32).astype(b16)
        gg_ref[:, cols] = both[:hidden_rows]
        gu_ref[:, cols] = both[hidden_rows:]

    def grads_out(n):
        cols = pl.ds(n * cut, cut)
        gd_ref[:, cols] = lax.dot_general(
            hps[...], db[:, cols], nn, preferred_element_type=f32
        ).astype(b16)

    for copy in mine:
        copy.wait()
    def send_table():
        for s in range(line):
            for dy in range(2):
                if s + dy:
                    push(
                        tab_own, tab_in.at[s, dy], (2 * across(z, s) + flipped(dy), h),
                        tab_send.at[s, dy], tab_recv.at[s, dy],
                    )

    def table_in(s):
        for dy in range(2):
            if s + dy:
                arrived(tab_in.at[s, dy], tab_recv.at[s, dy])

    def finish(s):
        middle(s)
        send_part(s)
        send_score(s)

    gather_own(0)
    send_plane(1)
    start_middle()
    send_table()
    weights = [
        local(wg_ref, wgu.at[pl.ds(0, hidden_rows)], w_sem.at[0]),
        local(wu_ref, wgu.at[pl.ds(hidden_rows, hidden_rows)], w_sem.at[1]),
        local(wd_ref, wdn, w_sem.at[2]),
    ]
    for r, ref in enumerate((wg_ref, wu_ref)):
        for n in range(4):
            q = 2 * (n % 2) + (c if n // 2 else 1 - c)
            weights.append(local(
                ref.at[:, pl.ds(pl.multiple_of(q * quarter, quarter), quarter)],
                wsides.at[pl.ds(r * hidden_rows, hidden_rows), pl.ds(n * quarter, quarter)],
                w_sem.at[5 + 4 * r + n],
            ))
    gather_first(0)
    relay_near()
    gather_own(1)
    gather_second(0, 2)
    gather_second(0, 3)
    gather_core(0)
    gather_own(2)
    send_rest(1)
    send_rest(3)
    for copy in weights:
        copy.wait()
    table_in(0)
    forward(0)
    gather_second(1, 2)
    finish(0)
    gather_first(2)
    gather_own(3)
    settle_core(0)
    gather_second(2, 2)
    gather_second(2, 3)
    gather_core(2)
    table_in(2)
    forward(2)
    gather_first(3)
    finish(2)
    gather_first(1)
    settle_core(2)
    gather_second(1, 3)
    gather_core(1)
    table_in(1)
    settle_first(0)
    forward(1)
    gather_second(3, 2)
    middle(1)
    send_part(1)
    gather_second(3, 3)
    settle_core(1)
    gather_core(3)
    table_in(3)
    forward(3)
    settle_first(2)
    middle(3)
    send_part(3)
    settle_second(0)
    settle_core(3)
    settle_second(2)
    settle_first(1)
    send_score(1)
    send_score(3)
    grads_in(0)
    grads_in(1)
    settle_first(3)
    grads_in(2)
    settle_second(1)
    grads_out(0)
    settle_second(3)
    grads_in(3)
    grads_out(1)
    grads_out(2)
    grads_out(3)

    for copy in owns:
        copy.wait()
    for s in range(line):
        for dy in range(2):
            for j in range(halves):
                if s + dy + j:
                    arrived(
                        back.at[s, dy, lax.rem(h + halves - j, halves)], score_recv.at[s, dy, j]
                    )
    total = jnp.zeros((top, rows), f32)
    for s in range(line):
        for dy in range(2):
            block = back[s, dy, 0]
            for j in range(1, halves):
                block = block + back[s, dy, j]
            first = local_exp * (2 * across(z, s) + flipped(dy))
            for l in range(local_exp):
                total = total + jnp.where(
                    route_t == first + l, block[l:l + 1, :], 0.0
                )
    gp_ref[...] = total
    for s in range(1, line):
        arrived(zin.at[s], last_recv.at[s])

    @row_loop(rows)
    def _(i):
        whole = fin[0, some(i)].astype(f32)
        for s in range(1, line):
            whole = whole + zin[s, some(i)].astype(f32)
        gt_ref[some(i)] = whole.astype(b16)

    for copy in sends:
        copy.wait_send()

    @pl.when(middle_chip)
    def _():
        for copy in passed:
            copy.wait_send()


def fused(tokens, cotangent, route, prob, wg, wu, wd, groups, halves, local_exp):
    rows, quarter = tokens.shape
    line, wide = groups // 2, quarter // 2
    hidden_rows, width = wg.shape
    experts, top = local_exp * groups, route.shape[0]
    b16, f32 = tokens.dtype, jnp.float32
    dma = pltpu.SemaphoreType.DMA
    vmem = pl.BlockSpec(memory_space=pltpu.VMEM)
    hbm = pl.BlockSpec(memory_space=pltpu.HBM)
    total = groups * rows
    grad = jax.ShapeDtypeStruct((hidden_rows, width), b16)
    return pl.pallas_call(
        functools.partial(fused_kernel, groups, halves, local_exp),
        out_shape=(
            jax.ShapeDtypeStruct((rows, quarter), b16),
            jax.ShapeDtypeStruct((top, rows), f32),
            grad, grad, grad,
        ),
        in_specs=[hbm] * 7,
        out_specs=[vmem] * 5,
        scratch_shapes=[
            pltpu.VMEM((total, width), b16),
            pltpu.VMEM((total, width), b16),
            pltpu.VMEM((2 * hidden_rows, width), b16),
            pltpu.VMEM((2 * hidden_rows, width), b16),
            pltpu.VMEM((hidden_rows, width), b16),
            pltpu.VMEM((2 * hidden_rows, 2 * rows), f32),
            pltpu.VMEM((hidden_rows, 2 * rows), f32),
            pltpu.VMEM((2 * hidden_rows, total), b16),
            pltpu.VMEM((hidden_rows, total), b16),
            pltpu.VMEM((2 * rows, 2 * hidden_rows), b16),
            pltpu.VMEM(route.shape, route.dtype),
            pltpu.VMEM(prob.shape, prob.dtype),
            pltpu.VMEM((experts, rows), f32),
            pltpu.VMEM((line, 2, experts, rows), f32),
            pltpu.VMEM((line, 2, 8, rows), f32),
            pltpu.VMEM((line, 2, halves, 8, rows), f32),
            pltpu.VMEM((line, 2, 2 * rows, quarter), b16),
            pltpu.VMEM((line, 2, 2 * rows, quarter), b16),
            pltpu.VMEM((line, 2, 2 * rows, quarter), b16),
            pltpu.VMEM((line, 2, 2, 2 * rows, wide), b16),
            pltpu.VMEM((line, 2 * rows, wide), b16),
            pltpu.VMEM((line, rows, wide), b16),
            pltpu.VMEM((line, 2, rows, wide), b16),
            pltpu.VMEM((line, rows, wide), b16),
            pltpu.VMEM((line, 2 * rows, wide), b16),
            pltpu.VMEM((line, 2, rows, wide), b16),
            pltpu.VMEM((line, rows, quarter), b16),
            pltpu.VMEM((line, rows, quarter), b16),
            dma((2, line)), dma((2, 2 * line)), dma((2, 4 * line)), dma((2, 2)), dma((2, 4)), dma((2, line)),
            dma((2, line)), dma((2, line)), dma((2, 2 * line)), dma((2, 4 * line)),
            dma((4,)), dma((13,)),
            dma((line, 2)), dma((line, 2)),
            dma((line, 2, halves)), dma((line, 2, halves)),
            dma((line, 2)), dma((line, 2)),
            dma((line, 4)), dma((line, 4)),
            dma((line,)), dma((line,)),
        ],
        compiler_params=pltpu.CompilerParams(
            collective_id=0, has_side_effects=True, vmem_limit_bytes=VMEM_BYTES
        ),
    )(tokens, cotangent, route, prob, wg, wu, wd)


def drain_kernel(count, *refs):
    sources, targets, sem = refs[:count], refs[count:2 * count], refs[2 * count]
    copies = [pltpu.make_async_copy(a, b, sem.at[i]) for i, (a, b) in enumerate(zip(sources, targets))]
    for copy in copies:
        copy.start()
    for copy in copies:
        copy.wait()


def drain(arrays):
    count = len(arrays)
    return pl.pallas_call(
        functools.partial(drain_kernel, count),
        out_shape=[jax.ShapeDtypeStruct(a.shape, a.dtype) for a in arrays],
        in_specs=[pl.BlockSpec(memory_space=pltpu.VMEM)] * count,
        out_specs=[pl.BlockSpec(memory_space=pl.ANY)] * count,
        scratch_shapes=[pltpu.SemaphoreType.DMA((count,))],
        compiler_params=pltpu.CompilerParams(vmem_limit_bytes=DRAIN_BYTES),
    )(*arrays)


def per_device(tokens, cotangent, route, prob, w_gate, w_up, w_down):
    tok_rows, quarter = tokens.shape
    local_exp, units, width = w_gate.shape
    groups = lax.axis_size("expert")
    halves = lax.axis_size("half")
    experts = local_exp * groups
    total = groups * tok_rows
    f32 = jnp.float32
    me = lax.axis_index("expert")

    fast = (
        groups == 2 * halves and halves == 2 * 2 and width == 4 * quarter
        and tok_rows == LANES and quarter % (2 * LANES) == 0
        and units % 32 == 0 and local_exp <= 8 and experts <= 2 * LANES and route.shape[1] <= 8
        and 2 * total * width * 2 + 12 * local_exp * units * width <= VMEM_BYTES // 2
    )
    if fast:
        flat = (local_exp * units, width)
        results = fused(
            *[pltpu.with_memory_space_constraint(v, pltpu.HBM) for v in (tokens, cotangent, route.T, prob.T)], w_gate.reshape(flat), w_up.reshape(flat),
            w_down.reshape(flat), groups, halves, local_exp,
        )
        grad_tokens, grad_prob, *grads = drain(results)
        grads = [g.reshape(local_exp, units, width) for g in grads]
        return (grad_tokens, grad_prob.T, *grads)

    hit = route[:, :, None] == jnp.arange(experts, dtype=route.dtype)
    table = jnp.sum(jnp.where(hit, prob[:, :, None], 0).astype(f32), axis=1).astype(prob.dtype)
    mine = lax.all_to_all(
        table.reshape(tok_rows, groups, local_exp), "expert",
        split_axis=1, concat_axis=0, tiled=True,
    ).reshape(total, local_exp)
    x = gather_all(tokens, groups, halves)
    d = gather_all(cotangent, groups, halves)
    weight = jnp.repeat(mine.astype(f32), units, axis=1)

    wg = w_gate.reshape(local_exp * units, width)
    wu = w_up.reshape(local_exp * units, width)
    wd = w_down.reshape(local_exp * units, width)
    nt = (((1,), (1,)), ((), ()))
    tn = (((0,), (0,)), ((), ()))
    gate = lax.dot_general(x, wg, nt, preferred_element_type=f32)
    upval = lax.dot_general(x, wu, nt, preferred_element_type=f32)
    raw = lax.dot_general(d, wd, nt, preferred_element_type=f32)
    sig = jax.nn.sigmoid(gate)
    act = gate * sig
    hidden = act * upval
    score = jnp.sum((hidden * raw).reshape(total, local_exp, units), axis=2)
    dact = weight * raw
    hp = (weight * hidden).astype(jnp.bfloat16)
    dgate = (dact * upval * sig * (1.0 + gate * (1.0 - sig))).astype(jnp.bfloat16)
    dup = (dact * act).astype(jnp.bfloat16)
    part = lax.dot_general(
        jnp.concatenate([dgate, dup], axis=1), jnp.concatenate([wg, wu], axis=0),
        (((1,), (0,)), ((), ())), preferred_element_type=f32,
    ).astype(jnp.bfloat16)
    part = part.reshape(groups, tok_rows, halves, quarter).transpose(0, 2, 1, 3)
    grad_tokens = lax.psum_scatter(
        part.reshape(groups * halves * tok_rows, quarter), BOTH,
        scatter_dimension=0, tiled=True,
    )
    sent = jnp.broadcast_to(
        score.reshape(groups, 1, tok_rows, local_exp), (groups, halves, tok_rows, local_exp)
    ).reshape(groups * halves, tok_rows * local_exp)
    back = lax.all_to_all(sent, BOTH, split_axis=0, concat_axis=0, tiled=True)
    back = jnp.sum(back.reshape(groups, halves, tok_rows, local_exp), axis=1)
    back = back.transpose(1, 0, 2).reshape(tok_rows, 1, experts)
    grad_prob = jnp.sum(jnp.where(hit, back, 0), axis=2)
    shape = (local_exp, units, width)
    grad_gate = lax.dot_general(dgate, x, tn, preferred_element_type=f32).astype(jnp.bfloat16)
    grad_up = lax.dot_general(dup, x, tn, preferred_element_type=f32).astype(jnp.bfloat16)
    grad_down = lax.dot_general(hp, d, tn, preferred_element_type=f32).astype(jnp.bfloat16)
    return (
        grad_tokens,
        grad_prob,
        grad_gate.reshape(shape),
        grad_up.reshape(shape),
        grad_down.reshape(shape),
    )


def solution(mesh):
    in_specs = (
        P("expert", "half"),
        P("expert", "half"),
        P("expert", None),
        P("expert", None),
        P("expert", "half", None),
        P("expert", "half", None),
        P("expert", "half", None),
    )
    out_specs = (
        P("expert", "half"),
        P("expert", None),
        P("expert", "half", None),
        P("expert", "half", None),
        P("expert", "half", None),
    )
    return jax.shard_map(
        per_device, mesh=mesh, in_specs=in_specs, out_specs=out_specs, check_vma=False
    )
```

```python
import functools

import jax
import jax.numpy as jnp
from jax import lax
from jax.experimental import pallas as pl
from jax.experimental.pallas import tpu as pltpu
from jax.sharding import PartitionSpec as P

BOTH = ("expert", "half")


def gather_all(block, groups, halves):
    rows, quarter = block.shape
    parts = lax.all_gather(block, BOTH, axis=0).reshape(groups, halves, rows, quarter)
    return parts.transpose(0, 2, 1, 3).reshape(groups * rows, halves * quarter)


LANES = 128
VMEM_BYTES = 48 << 20
DRAIN_BYTES = 1 << 20
MESH = pl.DeviceIdType.MESH


def place(groups):
    e, h = lax.axis_index("expert"), lax.axis_index("half")
    return lax.div(e, 2), lax.rem(e, 2), lax.div(h, 2), lax.rem(h, 2)


def across(z, step):
    bit = 1
    while bit <= step:
        if step & bit:
            z = z + bit * (1 - 2 * lax.rem(lax.div(z, bit), 2))
        bit *= 2
    return z


def greet(peers):
    barrier = pltpu.get_barrier_semaphore()
    for peer in peers:
        pl.semaphore_signal(barrier, inc=1, device_id=peer, device_id_type=MESH)
    pl.semaphore_wait(barrier, len(peers))


def fused_kernel(
    groups, halves, local_exp, tok_ref, cot_ref, route_ref, prob_ref, wg_ref, wu_ref, wd_ref,
    gt_ref, gp_ref, gg_ref, gu_ref, gd_ref,
    xb, db, wgu, wsides, wdn, gates, raws, dgu, hps, turned, route_in, prob_in, tab_own, tab_in, score, back,
    psend, own, cin, acc, xin0, yin0, yin1, xin1, t0, t1, fin, zin,
    first_send, second_send, core_send, rest_send, pass_send, z_send, z_sem, p_sem, q_sem, c_sem, own_sem, w_sem,
    tab_send, tab_recv, score_send, score_recv,
    part_send, part_recv, hop_send, hop_recv, last_send, last_recv,
):
    line = groups // 2
    z, y, x, c = place(groups)
    e, h = 2 * z + y, 2 * x + c
    rows, quarter = tok_ref.shape
    wide = quarter // 2
    hidden_rows, width = wg_ref.shape
    units = hidden_rows // local_exp
    experts = local_exp * groups
    top = route_ref.shape[0]
    f32, b16 = jnp.float32, tok_ref.dtype
    nt = (((1,), (1,)), ((), ()))
    nn = (((1,), (0,)), ((), ()))
    y_peer = (2 * z + 1 - y, h)
    x_peer = (e, 2 * (1 - x) + c)
    c_peer = (e, 2 * x + 1 - c)

    def local(src, dst, sem):
        copy = pltpu.make_async_copy(src, dst, sem)
        copy.start()
        return copy

    def slot(out, s, yy, xx, cc):
        row = pl.multiple_of((2 * s + yy) * rows, rows)
        col = pl.multiple_of((2 * xx + cc) * quarter, quarter)
        return out.at[pl.ds(row, rows), pl.ds(col, quarter)]

    pair = ((tok_ref, xb), (cot_ref, db))

    def at(a, s, kind, cc):
        over = (kind % 2, kind // 2) if a == 0 else (kind // 2, kind % 2)
        return slot(pair[a][1], s, 1 - y if over[0] else y, 1 - x if over[1] else x, cc)

    mine = [local(pair[a][0], at(a, 0, 0, c), own_sem.at[1 + a]) for a in range(2)]

    small = [local(route_ref, route_in, w_sem.at[3]), local(prob_ref, prob_in, w_sem.at[4])]
    for copy in small:
        copy.wait()
    route_t = route_in[...]
    prob_t = prob_in[...].astype(f32)
    row_of = lax.broadcasted_iota(jnp.int32, (experts, rows), 0)
    table = jnp.zeros((experts, rows), f32)
    for k in range(top):
        table = table + jnp.where(row_of == route_t[k:k + 1, :], prob_t[k:k + 1, :], 0.0)
    tab_own[...] = table
    tab_in[0, 0] = table

    greet([
        (lax.rem(e + i, groups), lax.rem(h + j, halves))
        for i in range(groups) for j in range(halves) if i + j
    ])
    sends, owns = [], []

    def push(src, dst, peer, number, sem):
        copy = pltpu.make_async_remote_copy(
            src_ref=src, dst_ref=dst, send_sem=number, recv_sem=sem,
            device_id=peer, device_id_type=MESH,
        )
        copy.start()
        sends.append(copy)
        return copy

    def arrived(dst, sem):
        pltpu.make_async_remote_copy(
            src_ref=dst, dst_ref=dst, send_sem=own_sem.at[0], recv_sem=sem,
            device_id=c_peer, device_id_type=MESH,
        ).wait_recv()

    hops = ((y_peer, x_peer), (x_peer, y_peer))

    def along(s):
        return (2 * across(z, s) + y, h)

    middle_chip = lax.div(z + 1, 2) == 1
    passed = []

    def pass_on(src, s_to, step, a, number):
        copy = pltpu.make_async_remote_copy(
            src_ref=src, dst_ref=at(a, s_to, 0, c), send_sem=pass_send.at[a, number],
            recv_sem=z_sem.at[a, s_to], device_id=along(step), device_id_type=MESH,
        )
        passed.append(copy)
        return copy

    def start_middle():
        copies = [pass_on(at(a, 0, 0, c), 3, 3, a, 0) for a in range(2)]

        @pl.when(middle_chip)
        def _():
            for copy in copies:
                copy.start()

    def relay_near():
        inner = [pass_on(at(a, 1, 0, c), 2, 3, a, 1) for a in range(2)]
        outer = [pass_on(at(a, 3, 0, c), 2, 1, a, 2) for a in range(2)]

        @pl.when(middle_chip)
        def _():
            for a in range(2):
                arrived(at(a, 1, 0, c), z_sem.at[a, 1])
                inner[a].start()
                arrived(at(a, 3, 0, c), z_sem.at[a, 3])
                outer[a].start()

    def gather_own(s):
        have = [at(a, s, 0, c) for a in range(2)]
        far = [pass_on(at(a, 2, 0, c), 3, 1, a, 3) for a in range(2)] if s == 2 else None
        for a in range(2):
            if s == 2:
                arrived(have[a], z_sem.at[a, s])

                @pl.when(middle_chip)
                def _():
                    far[a].start()
            elif s > 0:
                @pl.when(jnp.logical_not(middle_chip))
                def _():
                    arrived(have[a], z_sem.at[a, s])
            if s != 1:
                push(have[a], have[a], hops[a][0], first_send.at[a, s], p_sem.at[a, s])
            if s > 0:
                push(have[a], have[a], hops[a][1], second_send.at[a, s], q_sem.at[a, s])
        for a in range(2):
            if s == 0:
                push(have[a], have[a], hops[a][1], second_send.at[a, s], q_sem.at[a, s])
        for a in range(2):
            push(have[a], have[a], c_peer, core_send.at[a, s], c_sem.at[a, s])

    def gather_first(s):
        there = [at(a, s, 1, c) for a in range(2)]
        for a in range(2):
            arrived(there[a], p_sem.at[a, s])
            if s != 1:
                push(
                    there[a], there[a], hops[a][1],
                    second_send.at[a, line + s], q_sem.at[a, line + s],
                )
        for a in range(2):
            push(there[a], there[a], c_peer, core_send.at[a, line + s], c_sem.at[a, line + s])

    def gather_second(s, kind):
        for a in range(2):
            there = at(a, s, kind, c)
            arrived(there, q_sem.at[a, (kind - 2) * line + s])
            push(there, there, c_peer, core_send.at[a, kind * line + s], c_sem.at[a, kind * line + s])

    def send_plane(s):
        for a in range(2):
            push(at(a, 0, 0, c), at(a, s, 0, c), along(s), z_send.at[a, s], z_sem.at[a, s])

    def send_rest(kind):
        for a in range(2):
            sem = p_sem.at[a, 1] if kind == 1 else q_sem.at[a, line + 1]
            push(at(a, 0, kind, c), at(a, 1, kind, c), along(1), rest_send.at[a, kind // 2], sem)

    def gather_core(s):
        for a in range(2):
            for kind in range(4):
                arrived(at(a, s, kind, 1 - c), c_sem.at[a, kind * line + s])

    def plane(s):
        return pl.ds(2 * s * rows, 2 * rows)

    def forward(s):
        for r in range(2):
            part = pl.ds(r * hidden_rows, hidden_rows)
            gates[part, :] = lax.dot_general(
                wgu[part, :], xb[plane(s), :], nt, preferred_element_type=f32
            )

    def middle(s):
        for r in range(2):
            part = pl.ds(r * hidden_rows // 2, hidden_rows // 2)
            raws[part, :] = lax.dot_general(
                wdn[part, :], db[plane(s), :], nt, preferred_element_type=f32
            )
        chunk = 32 if units % 32 == 0 else 16
        expert_of = lax.broadcasted_iota(jnp.int32, (experts, rows), 0)
        lane = pl.ds(2 * s * rows, 2 * rows)
        sums = []
        tabs = [tab_in[s, y], tab_in[s, 1 - y]]
        for l in range(local_exp):
            weight = jnp.concatenate([
                jnp.sum(jnp.where(expert_of == local_exp * e + l, t, 0.0), axis=0, keepdims=True)
                for t in tabs
            ], axis=1)

            def step(i, total, l=l, weight=weight):
                at_row = pl.multiple_of(l * units + i * chunk, chunk)
                up_row = pl.multiple_of(hidden_rows + l * units + i * chunk, chunk)
                g = gates[pl.ds(at_row, chunk), :]
                u = gates[pl.ds(up_row, chunk), :]
                r = raws[pl.ds(at_row, chunk), :]
                sig = jax.nn.sigmoid(g)
                act = g * sig
                hidden = act * u
                dact = weight * r
                hps[pl.ds(at_row, chunk), lane] = (weight * hidden).astype(b16)
                dgu[pl.ds(at_row, chunk), lane] = (
                    dact * u * sig * (1.0 + g * (1.0 - sig))
                ).astype(b16)
                dgu[pl.ds(up_row, chunk), lane] = (dact * act).astype(b16)
                return total + jnp.sum((hidden * r).reshape(chunk // 8, 8, 2 * rows), axis=0)

            total = lax.fori_loop(0, units // chunk, step, jnp.zeros((8, 2 * rows), f32))
            sums.append(jnp.sum(total, axis=0, keepdims=True))
        sub = lax.broadcasted_iota(jnp.int32, (8, rows), 0)
        for yy in range(2):
            block = jnp.zeros((8, rows), f32)
            for l in range(local_exp):
                block = jnp.where(sub == l, sums[l][:, yy * rows:(yy + 1) * rows], block)
            score[s, yy] = block
        turned[...] = dgu[:, lane].T

    def part_of(side):
        cols = pl.ds(side * 2 * quarter, 2 * quarter)
        return lax.dot_general(
            turned[...], wsides[:, cols], nn, preferred_element_type=f32
        ).astype(b16)

    def send_part(s):
        theirs = part_of(0)
        for xx in range(2):
            psend[s, xx] = theirs[:, xx * quarter:(xx + 1) * quarter]
            push(psend.at[s, xx], cin.at[s, xx], c_peer, part_send.at[s, xx], part_recv.at[s, xx])
        mine = part_of(1)
        for xx in range(2):
            own[s, xx] = mine[:, xx * quarter:(xx + 1) * quarter]

    def flipped(dy):
        return 1 - y if dy else y

    def send_score(s):
        for dy in range(2):
            for j in range(halves):
                if s + dy + j == 0:
                    owns.append(local(score.at[0, y], back.at[0, 0, h], own_sem.at[3]))
                    continue
                push(
                    score.at[s, flipped(dy)], back.at[s, dy, h],
                    (2 * across(z, s) + flipped(dy), lax.rem(h + j, halves)),
                    score_send.at[s, dy, j], score_recv.at[s, dy, j],
                )

    step_rows = 32

    def row_loop(count):
        return pl.loop(0, count // step_rows)

    def some(i):
        return pl.ds(pl.multiple_of(i * step_rows, step_rows), step_rows)

    def settle_core(s):
        for xx in range(2):
            arrived(cin.at[s, xx], part_recv.at[s, xx])

            @row_loop(2 * rows)
            def _(i):
                both = own[s, xx, some(i)].astype(f32) + cin[s, xx, some(i)].astype(f32)
                acc[s, 0, xx, some(i)] = both[:, :wide].astype(b16)
                acc[s, 1, xx, some(i)] = both[:, wide:].astype(b16)

        push(acc.at[s, 0, 1 - x], xin0.at[s], x_peer, hop_send.at[s, 0], hop_recv.at[s, 0])
        away = pl.ds(pl.multiple_of((1 - y) * rows, rows), rows)
        push(acc.at[s, 1, :, away], yin1.at[s], y_peer, hop_send.at[s, 1], hop_recv.at[s, 1])

    def settle_first(s):
        arrived(xin0.at[s], hop_recv.at[s, 0])

        @row_loop(2 * rows)
        def _(i):
            t0[s, some(i)] = (
                acc[s, 0, x, some(i)].astype(f32) + xin0[s, some(i)].astype(f32)
            ).astype(b16)

        away = pl.ds(pl.multiple_of((1 - y) * rows, rows), rows)
        push(t0.at[s, away], yin0.at[s], y_peer, hop_send.at[s, 2], hop_recv.at[s, 2])
        arrived(yin1.at[s], hop_recv.at[s, 1])

        @row_loop(rows)
        def _(i):
            here = pl.ds(pl.multiple_of(y * rows + i * step_rows, step_rows), step_rows)
            for xx in range(2):
                t1[s, xx, some(i)] = (
                    acc[s, 1, xx, here].astype(f32) + yin1[s, xx, some(i)].astype(f32)
                ).astype(b16)

        push(t1.at[s, 1 - x], xin1.at[s], x_peer, hop_send.at[s, 3], hop_recv.at[s, 3])

    def settle_second(s):
        arrived(yin0.at[s], hop_recv.at[s, 2])
        arrived(xin1.at[s], hop_recv.at[s, 3])

        @row_loop(rows)
        def _(i):
            here = pl.ds(pl.multiple_of(y * rows + i * step_rows, step_rows), step_rows)
            fin[s, some(i), :wide] = (
                t0[s, here].astype(f32) + yin0[s, some(i)].astype(f32)
            ).astype(b16)
            fin[s, some(i), wide:] = (
                t1[s, x, some(i)].astype(f32) + xin1[s, some(i)].astype(f32)
            ).astype(b16)

        if s > 0:
            push(fin.at[s], zin.at[s], (2 * across(z, s) + y, h), last_send.at[s], last_recv.at[s])

    cut = quarter

    def grads_in(n):
        cols = pl.ds(n * cut, cut)
        both = lax.dot_general(dgu[...], xb[:, cols], nn, preferred_element_type=f32).astype(b16)
        gg_ref[:, cols] = both[:hidden_rows]
        gu_ref[:, cols] = both[hidden_rows:]

    def grads_out(n):
        cols = pl.ds(n * cut, cut)
        gd_ref[:, cols] = lax.dot_general(
            hps[...], db[:, cols], nn, preferred_element_type=f32
        ).astype(b16)

    for copy in mine:
        copy.wait()
    def send_table():
        for s in range(line):
            for dy in range(2):
                if s + dy:
                    push(
                        tab_own, tab_in.at[s, dy], (2 * across(z, s) + flipped(dy), h),
                        tab_send.at[s, dy], tab_recv.at[s, dy],
                    )

    def table_in(s):
        for dy in range(2):
            if s + dy:
                arrived(tab_in.at[s, dy], tab_recv.at[s, dy])

    def finish(s):
        middle(s)
        send_part(s)
        send_score(s)

    gather_own(0)
    send_plane(1)
    start_middle()
    send_table()
    weights = [
        local(wg_ref, wgu.at[pl.ds(0, hidden_rows)], w_sem.at[0]),
        local(wu_ref, wgu.at[pl.ds(hidden_rows, hidden_rows)], w_sem.at[1]),
        local(wd_ref, wdn, w_sem.at[2]),
    ]
    for r, ref in enumerate((wg_ref, wu_ref)):
        for n in range(4):
            q = 2 * (n % 2) + (c if n // 2 else 1 - c)
            weights.append(local(
                ref.at[:, pl.ds(pl.multiple_of(q * quarter, quarter), quarter)],
                wsides.at[pl.ds(r * hidden_rows, hidden_rows), pl.ds(n * quarter, quarter)],
                w_sem.at[5 + 4 * r + n],
            ))
    gather_first(0)
    relay_near()
    gather_own(1)
    gather_second(0, 2)
    gather_second(0, 3)
    gather_core(0)
    gather_own(2)
    send_rest(1)
    send_rest(3)
    for copy in weights:
        copy.wait()
    table_in(0)
    forward(0)
    gather_second(1, 2)
    finish(0)
    gather_first(2)
    gather_own(3)
    gather_second(2, 2)
    gather_second(2, 3)
    gather_core(2)
    table_in(2)
    forward(2)
    gather_first(3)
    finish(2)
    gather_first(1)
    settle_core(2)
    settle_core(0)
    gather_second(1, 3)
    gather_core(1)
    table_in(1)
    forward(1)
    gather_second(3, 2)
    middle(1)
    send_part(1)
    gather_second(3, 3)
    settle_core(1)
    gather_core(3)
    table_in(3)
    forward(3)
    settle_first(2)
    middle(3)
    settle_first(0)
    send_part(3)
    settle_core(3)
    settle_second(2)
    settle_first(1)
    send_score(1)
    send_score(3)
    grads_in(0)
    grads_in(1)
    settle_first(3)
    grads_in(2)
    settle_second(1)
    grads_out(0)
    settle_second(3)
    grads_in(3)
    grads_out(1)
    grads_out(2)
    grads_out(3)
    settle_second(0)

    for copy in owns:
        copy.wait()
    for s in range(line):
        for dy in range(2):
            for j in range(halves):
                if s + dy + j:
                    arrived(
                        back.at[s, dy, lax.rem(h + halves - j, halves)], score_recv.at[s, dy, j]
                    )
    total = jnp.zeros((top, rows), f32)
    for s in range(line):
        for dy in range(2):
            block = back[s, dy, 0]
            for j in range(1, halves):
                block = block + back[s, dy, j]
            first = local_exp * (2 * across(z, s) + flipped(dy))
            for l in range(local_exp):
                total = total + jnp.where(
                    route_t == first + l, block[l:l + 1, :], 0.0
                )
    gp_ref[...] = total
    for s in range(1, line):
        arrived(zin.at[s], last_recv.at[s])

    @row_loop(rows)
    def _(i):
        whole = fin[0, some(i)].astype(f32)
        for s in range(1, line):
            whole = whole + zin[s, some(i)].astype(f32)
        gt_ref[some(i)] = whole.astype(b16)

    for copy in sends:
        copy.wait_send()

    @pl.when(middle_chip)
    def _():
        for copy in passed:
            copy.wait_send()


def fused(tokens, cotangent, route, prob, wg, wu, wd, groups, halves, local_exp):
    rows, quarter = tokens.shape
    line, wide = groups // 2, quarter // 2
    hidden_rows, width = wg.shape
    experts, top = local_exp * groups, route.shape[0]
    b16, f32 = tokens.dtype, jnp.float32
    dma = pltpu.SemaphoreType.DMA
    vmem = pl.BlockSpec(memory_space=pltpu.VMEM)
    hbm = pl.BlockSpec(memory_space=pltpu.HBM)
    total = groups * rows
    grad = jax.ShapeDtypeStruct((hidden_rows, width), b16)
    return pl.pallas_call(
        functools.partial(fused_kernel, groups, halves, local_exp),
        out_shape=(
            jax.ShapeDtypeStruct((rows, quarter), b16),
            jax.ShapeDtypeStruct((top, rows), f32),
            grad, grad, grad,
        ),
        in_specs=[hbm] * 7,
        out_specs=[vmem] * 5,
        scratch_shapes=[
            pltpu.VMEM((total, width), b16),
            pltpu.VMEM((total, width), b16),
            pltpu.VMEM((2 * hidden_rows, width), b16),
            pltpu.VMEM((2 * hidden_rows, width), b16),
            pltpu.VMEM((hidden_rows, width), b16),
            pltpu.VMEM((2 * hidden_rows, 2 * rows), f32),
            pltpu.VMEM((hidden_rows, 2 * rows), f32),
            pltpu.VMEM((2 * hidden_rows, total), b16),
            pltpu.VMEM((hidden_rows, total), b16),
            pltpu.VMEM((2 * rows, 2 * hidden_rows), b16),
            pltpu.VMEM(route.shape, route.dtype),
            pltpu.VMEM(prob.shape, prob.dtype),
            pltpu.VMEM((experts, rows), f32),
            pltpu.VMEM((line, 2, experts, rows), f32),
            pltpu.VMEM((line, 2, 8, rows), f32),
            pltpu.VMEM((line, 2, halves, 8, rows), f32),
            pltpu.VMEM((line, 2, 2 * rows, quarter), b16),
            pltpu.VMEM((line, 2, 2 * rows, quarter), b16),
            pltpu.VMEM((line, 2, 2 * rows, quarter), b16),
            pltpu.VMEM((line, 2, 2, 2 * rows, wide), b16),
            pltpu.VMEM((line, 2 * rows, wide), b16),
            pltpu.VMEM((line, rows, wide), b16),
            pltpu.VMEM((line, 2, rows, wide), b16),
            pltpu.VMEM((line, rows, wide), b16),
            pltpu.VMEM((line, 2 * rows, wide), b16),
            pltpu.VMEM((line, 2, rows, wide), b16),
            pltpu.VMEM((line, rows, quarter), b16),
            pltpu.VMEM((line, rows, quarter), b16),
            dma((2, line)), dma((2, 2 * line)), dma((2, 4 * line)), dma((2, 2)), dma((2, 4)), dma((2, line)),
            dma((2, line)), dma((2, line)), dma((2, 2 * line)), dma((2, 4 * line)),
            dma((4,)), dma((13,)),
            dma((line, 2)), dma((line, 2)),
            dma((line, 2, halves)), dma((line, 2, halves)),
            dma((line, 2)), dma((line, 2)),
            dma((line, 4)), dma((line, 4)),
            dma((line,)), dma((line,)),
        ],
        compiler_params=pltpu.CompilerParams(
            collective_id=0, has_side_effects=True, vmem_limit_bytes=VMEM_BYTES
        ),
    )(tokens, cotangent, route, prob, wg, wu, wd)


def drain_kernel(count, *refs):
    sources, targets, sem = refs[:count], refs[count:2 * count], refs[2 * count]
    copies = [pltpu.make_async_copy(a, b, sem.at[i]) for i, (a, b) in enumerate(zip(sources, targets))]
    for copy in copies:
        copy.start()
    for copy in copies:
        copy.wait()


def drain(arrays):
    count = len(arrays)
    return pl.pallas_call(
        functools.partial(drain_kernel, count),
        out_shape=[jax.ShapeDtypeStruct(a.shape, a.dtype) for a in arrays],
        in_specs=[pl.BlockSpec(memory_space=pltpu.VMEM)] * count,
        out_specs=[pl.BlockSpec(memory_space=pl.ANY)] * count,
        scratch_shapes=[pltpu.SemaphoreType.DMA((count,))],
        compiler_params=pltpu.CompilerParams(vmem_limit_bytes=DRAIN_BYTES),
    )(*arrays)


def per_device(tokens, cotangent, route, prob, w_gate, w_up, w_down):
    tok_rows, quarter = tokens.shape
    local_exp, units, width = w_gate.shape
    groups = lax.axis_size("expert")
    halves = lax.axis_size("half")
    experts = local_exp * groups
    total = groups * tok_rows
    f32 = jnp.float32
    me = lax.axis_index("expert")

    fast = (
        groups == 2 * halves and halves == 2 * 2 and width == 4 * quarter
        and tok_rows == LANES and quarter % (2 * LANES) == 0
        and units % 32 == 0 and local_exp <= 8 and experts <= 2 * LANES and route.shape[1] <= 8
        and 2 * total * width * 2 + 12 * local_exp * units * width <= VMEM_BYTES // 2
    )
    if fast:
        flat = (local_exp * units, width)
        results = fused(
            *[pltpu.with_memory_space_constraint(v, pltpu.HBM) for v in (tokens, cotangent, route.T, prob.T)], w_gate.reshape(flat), w_up.reshape(flat),
            w_down.reshape(flat), groups, halves, local_exp,
        )
        grad_tokens, grad_prob, *grads = drain(results)
        grads = [g.reshape(local_exp, units, width) for g in grads]
        return (grad_tokens, grad_prob.T, *grads)

    hit = route[:, :, None] == jnp.arange(experts, dtype=route.dtype)
    table = jnp.sum(jnp.where(hit, prob[:, :, None], 0).astype(f32), axis=1).astype(prob.dtype)
    mine = lax.all_to_all(
        table.reshape(tok_rows, groups, local_exp), "expert",
        split_axis=1, concat_axis=0, tiled=True,
    ).reshape(total, local_exp)
    x = gather_all(tokens, groups, halves)
    d = gather_all(cotangent, groups, halves)
    weight = jnp.repeat(mine.astype(f32), units, axis=1)

    wg = w_gate.reshape(local_exp * units, width)
    wu = w_up.reshape(local_exp * units, width)
    wd = w_down.reshape(local_exp * units, width)
    nt = (((1,), (1,)), ((), ()))
    tn = (((0,), (0,)), ((), ()))
    gate = lax.dot_general(x, wg, nt, preferred_element_type=f32)
    upval = lax.dot_general(x, wu, nt, preferred_element_type=f32)
    raw = lax.dot_general(d, wd, nt, preferred_element_type=f32)
    sig = jax.nn.sigmoid(gate)
    act = gate * sig
    hidden = act * upval
    score = jnp.sum((hidden * raw).reshape(total, local_exp, units), axis=2)
    dact = weight * raw
    hp = (weight * hidden).astype(jnp.bfloat16)
    dgate = (dact * upval * sig * (1.0 + gate * (1.0 - sig))).astype(jnp.bfloat16)
    dup = (dact * act).astype(jnp.bfloat16)
    part = lax.dot_general(
        jnp.concatenate([dgate, dup], axis=1), jnp.concatenate([wg, wu], axis=0),
        (((1,), (0,)), ((), ())), preferred_element_type=f32,
    ).astype(jnp.bfloat16)
    part = part.reshape(groups, tok_rows, halves, quarter).transpose(0, 2, 1, 3)
    grad_tokens = lax.psum_scatter(
        part.reshape(groups * halves * tok_rows, quarter), BOTH,
        scatter_dimension=0, tiled=True,
    )
    sent = jnp.broadcast_to(
        score.reshape(groups, 1, tok_rows, local_exp), (groups, halves, tok_rows, local_exp)
    ).reshape(groups * halves, tok_rows * local_exp)
    back = lax.all_to_all(sent, BOTH, split_axis=0, concat_axis=0, tiled=True)
    back = jnp.sum(back.reshape(groups, halves, tok_rows, local_exp), axis=1)
    back = back.transpose(1, 0, 2).reshape(tok_rows, 1, experts)
    grad_prob = jnp.sum(jnp.where(hit, back, 0), axis=2)
    shape = (local_exp, units, width)
    grad_gate = lax.dot_general(dgate, x, tn, preferred_element_type=f32).astype(jnp.bfloat16)
    grad_up = lax.dot_general(dup, x, tn, preferred_element_type=f32).astype(jnp.bfloat16)
    grad_down = lax.dot_general(hp, d, tn, preferred_element_type=f32).astype(jnp.bfloat16)
    return (
        grad_tokens,
        grad_prob,
        grad_gate.reshape(shape),
        grad_up.reshape(shape),
        grad_down.reshape(shape),
    )


def solution(mesh):
    in_specs = (
        P("expert", "half"),
        P("expert", "half"),
        P("expert", None),
        P("expert", None),
        P("expert", "half", None),
        P("expert", "half", None),
        P("expert", "half", None),
    )
    out_specs = (
        P("expert", "half"),
        P("expert", None),
        P("expert", "half", None),
        P("expert", "half", None),
        P("expert", "half", None),
    )
    return jax.shard_map(
        per_device, mesh=mesh, in_specs=in_specs, out_specs=out_specs, check_vma=False
    )
```
